128 devices in a mesh: wide: 8 (over x, y_hi), narrow: 16 (over y_lo, z, core).
Axes of the slice: x: 4, y: 4 (y_hi: 2, y_lo: 2; y = y_hi * 2 + y_lo), z: 4, core: 2. Of those that a mesh axis runs over, the one named last changes fastest.
Arguments:
- mixture: bfloat16 [4, 256, 256, 256], P(None, ('wide', 'narrow')), may hold values from -30 to 30
- w_attn: bfloat16 [2, 4, 256, 256], replicated, may hold values from -2.625 to 2.625
- w_up: bfloat16 [2, 256, 1024], replicated, may hold values from -0.375 to 0.375
- w_down: bfloat16 [2, 1024, 256], replicated, may hold values from -0.1875 to 0.1875
- norm_gain: float32 [2, 2, 256], replicated, may hold values from 0.1 to 1.9
- norm_bias: float32 [2, 2, 256], replicated, may hold values from -3 to 3
- group_gain: float32 [2, 256], replicated, may hold values from 0.1 to 1.9
- group_bias: float32 [2, 256], replicated, may hold values from -3 to 3
Outputs:
- separated: bfloat16 [4, 256, 256, 256], P(None, ('wide', 'narrow'))
The draws below stay inside these ranges and needn't reach their ends.
All inputs are finite; a program needn't handle non-finite values.
Results may differ from the reference program's by a relative error of at most 0.0083.
Values may be sent and summed in bfloat16 or wider, within the bound.
A program may use at most 64 MiB of HBM per device.

```python
import math
import jax
import jax.numpy as jnp
from jax import lax

D = 256
HEADS = 8
FF = 1024
FRAMES = 256
MIX = 4
SEGMENTS = 256
N_WIDE = 8


def draw_mixture(key, part):
    keys = jax.random.split(jax.random.fold_in(key, 11), 5)
    seg_positions = jnp.arange(SEGMENTS, dtype=jnp.float32)
    frame_positions = jnp.arange(FRAMES, dtype=jnp.float32)
    period = SEGMENTS // N_WIDE
    residue_level = jnp.exp(jax.random.uniform(keys[0], (MIX, period), minval=math.log(0.05), maxval=0.0))
    loudness = jnp.tile(residue_level, (1, N_WIDE))
    loudness = loudness * jnp.exp(jax.random.uniform(keys[1], (MIX, SEGMENTS), minval=math.log(0.7), maxval=math.log(1.2)))
    loudness = loudness * jnp.exp(math.log(3.0) * (seg_positions / SEGMENTS - 0.5))
    frame_ramp = jnp.exp(math.log(3.0) * (frame_positions / FRAMES - 0.5))
    channel_scale = jnp.exp(jax.random.uniform(keys[2], (D,), minval=math.log(0.4), maxval=math.log(2.0)))
    colour = 0.6 * jnp.clip(jax.random.normal(keys[3], (MIX, SEGMENTS, D)), -4.0, 4.0)
    entries = jnp.clip(jax.random.normal(keys[4], (MIX, SEGMENTS, FRAMES, D)), -3.0, 3.0)
    seg_offset = 0.8 * seg_positions / SEGMENTS
    frame_offset = 0.8 * frame_positions / FRAMES
    values = entries * loudness[:, :, None, None] * frame_ramp[None, None, :, None] * channel_scale
    values = values + colour[:, :, None, :] + seg_offset[None, :, None, None] + frame_offset[None, None, :, None]
    return values.astype(jnp.bfloat16)


def draw_w_attn(key, part):
    first_key = jax.random.fold_in(jax.random.fold_in(key, 23), 0)
    base_draw = jnp.clip(jax.random.normal(first_key, (2, 4, D, D)), -4.0, 4.0) / math.sqrt(D)
    return base_draw.astype(jnp.bfloat16)


def gaussian(own_key, shape, width, bound, kind=jnp.bfloat16):
    values = width * jax.random.normal(own_key, shape, jnp.float32)
    return jnp.clip(values, min=-bound, max=bound).astype(kind)


def setup_inputs(seed: int = 0) -> dict:
    splits = jax.random.split(jax.random.key(seed), 9)
    return {
        "mixture": draw_mixture(jax.random.fold_in(splits[8], 71), 0),
        "w_attn": draw_w_attn(jax.random.fold_in(splits[8], 71), 0),
        "w_up": gaussian(splits[2], (2, D, FF), D ** -0.5, 0.375),
        "w_down": gaussian(splits[3], (2, FF, D), FF ** -0.5, 0.1875),
        "norm_gain": jnp.clip(1.0 + 0.18 * jax.random.normal(splits[4], (2, 2, D), jnp.float32), 0.1, 1.9),
        "norm_bias": gaussian(splits[5], (2, 2, D), 0.5, 3.0, jnp.float32),
        "group_gain": jnp.clip(1.0 + 0.18 * jax.random.normal(splits[6], (2, D), jnp.float32), 0.1, 1.9),
        "group_bias": gaussian(splits[7], (2, D), 0.5, 3.0, jnp.float32),
    }


EPSILON = 1e-05

def positions_table(seq_length, model_width):
    positions = jnp.arange(seq_length, dtype=jnp.float32)[:, None]
    freq_index = jnp.arange(model_width // 2, dtype=jnp.float32)[None, :]
    angles = positions * jnp.exp(freq_index * (-2.0 * math.log(10000.0) / model_width))
    return jnp.concatenate([jnp.sin(angles), jnp.cos(angles)], axis=1)

def layer_norm(values, gain_row, bias_row):
    mean_value = lax.optimization_barrier(jnp.mean(values, axis=-1, keepdims=True))
    centered = values - mean_value
    variance = lax.optimization_barrier(jnp.mean(centered * centered, axis=-1, keepdims=True))
    return centered * lax.rsqrt(variance + EPSILON) * gain_row + bias_row

def encoder_block(seq_block, pos_table, attn_weights, up_weight, down_weight, gains, biases):
    groups, seq_length, inner_count, model_width = seq_block.shape
    head_size = model_width // HEADS
    state_rows = seq_block.astype(jnp.float32) + pos_table[None, :, None, :]
    normed = layer_norm(state_rows, gains[0], biases[0]).astype(jnp.bfloat16).reshape(-1, model_width)

    def project(matrix):
        product = jnp.dot(normed, matrix, preferred_element_type=jnp.float32).astype(jnp.bfloat16)
        return product.reshape(groups, seq_length, inner_count, HEADS, head_size)
    queries = project(attn_weights[0])
    key_rows = project(attn_weights[1])
    value_rows = project(attn_weights[2])
    scores = jnp.einsum('alnhe,amnhe->anhlm', queries.astype(jnp.float32), key_rows.astype(jnp.float32))
    scores = scores * (1.0 / math.sqrt(head_size))
    shifted = jnp.exp(scores - lax.optimization_barrier(jnp.max(scores, axis=-1, keepdims=True)))
    weights = (shifted / lax.optimization_barrier(jnp.sum(shifted, axis=-1, keepdims=True))).astype(jnp.bfloat16)
    attended = jnp.einsum('anhlm,amnhe->alnhe', weights.astype(jnp.float32), value_rows.astype(jnp.float32))
    attended = attended.astype(jnp.bfloat16).reshape(-1, model_width)
    mixed = jnp.dot(attended, attn_weights[3], preferred_element_type=jnp.float32)
    state_after = state_rows + mixed.reshape(state_rows.shape)
    normed_two = layer_norm(state_after, gains[1], biases[1]).astype(jnp.bfloat16).reshape(-1, model_width)
    hidden = jax.nn.relu(jnp.dot(normed_two, up_weight, preferred_element_type=jnp.float32)).astype(jnp.bfloat16)
    output = jnp.dot(hidden, down_weight, preferred_element_type=jnp.float32)
    return state_after + output.reshape(state_after.shape)

def run_layer(seq_data, layer_index, w_attn, w_up, w_down, norm_gain, norm_bias, block_rows):
    seq_count, seq_length, inner_count, model_width = seq_data.shape
    per_block = math.gcd(seq_count, max(1, block_rows // (seq_length * inner_count)))
    pos_table = positions_table(seq_length, model_width)
    blocked = seq_data.reshape(seq_count // per_block, per_block, seq_length, inner_count, model_width)

    def apply_block(seq_block):
        return encoder_block(seq_block, pos_table, w_attn[layer_index], w_up[layer_index], w_down[layer_index], norm_gain[layer_index], norm_bias[layer_index])
    return lax.map(apply_block, blocked).reshape(seq_count, seq_length, inner_count, model_width)

def group_norm(values, gain_row, bias_row):
    cell_count = values.shape[1] * values.shape[2] * values.shape[3]
    mean_value = lax.optimization_barrier(jnp.sum(values, axis=(1, 2, 3), keepdims=True)) / cell_count
    centered = values - mean_value
    variance = lax.optimization_barrier(jnp.sum(centered * centered, axis=(1, 2, 3), keepdims=True)) / cell_count
    return centered * lax.rsqrt(variance + EPSILON) * gain_row + bias_row

def reference(mixture, w_attn, w_up, w_down, norm_gain, norm_bias, group_gain, group_bias):
    mix_count, seg_count, frame_count, model_width = mixture.shape
    intra_out = run_layer(mixture.reshape(mix_count * seg_count, frame_count, 1, model_width), 0, w_attn, w_up, w_down, norm_gain, norm_bias, 8192).reshape(mixture.shape)
    carried = (group_norm(intra_out, group_gain[0], group_bias[0]) + mixture.astype(jnp.float32)).astype(jnp.bfloat16)
    turned = jnp.transpose(carried, (0, 2, 1, 3)).reshape(mix_count * frame_count, seg_count, 1, model_width)
    inter_out = run_layer(turned, 1, w_attn, w_up, w_down, norm_gain, norm_bias, 8192).astype(jnp.bfloat16)
    inter_out = jnp.transpose(inter_out.reshape(mix_count, frame_count, seg_count, model_width), (0, 2, 1, 3))
    separated = group_norm(inter_out.astype(jnp.float32), group_gain[1], group_bias[1]) + carried.astype(jnp.float32)
    return separated.astype(jnp.bfloat16)
```

```python
import math

import jax
import jax.numpy as jnp
import numpy as np
from jax import lax
from jax.experimental import pallas as pl
from jax.experimental.pallas import tpu as pltpu
from jax.sharding import PartitionSpec as P

F32 = jnp.float32
BF = jnp.bfloat16
MESH = pl.DeviceIdType.MESH

HEADS = 8
HEAD = 32
D = 256
LENGTH = 256
MIX = 4
PLANE = 16
COLUMN = 8
EPSILON = 1e-05
QUERY_SCALE = math.log2(math.e) / math.sqrt(HEAD)
SEQ_CELLS = float(LENGTH * D)
UNIT_CELLS = 2.0 * SEQ_CELLS
COLUMN_CELLS = UNIT_CELLS * COLUMN
MIX_CELLS = COLUMN_CELLS * PLANE


def position_tables():
    positions = np.arange(LENGTH, dtype=np.float32)[:, None]
    freq = np.arange(D // 2, dtype=np.float32)[None, :]
    angles = positions * np.exp(freq * np.float32(-2.0 * math.log(10000.0) / D))
    table = np.concatenate([np.sin(angles), np.cos(angles)], axis=1).astype(np.float32)
    r, p, s = np.meshgrid(np.arange(COLUMN), np.arange(PLANE), np.arange(2), indexing="ij")
    order = (16 * p + 2 * r + s).reshape(-1)
    return np.stack([table, table[order]])


def dot(a, b):
    return jnp.dot(a, b, preferred_element_type=F32)


def layer_norm(rows, gain, bias):
    mean = jnp.mean(rows, axis=-1, keepdims=True)
    centered = rows - mean
    variance = jnp.mean(centered * centered, axis=-1, keepdims=True)
    return centered * lax.rsqrt(variance + EPSILON) * gain + bias


def encoder(state, gains, biases, qv_t, wk, wo, up, down):
    normed = layer_norm(state, gains[0:1], biases[0:1]).astype(BF)
    both = lax.dot_general(qv_t, normed, (((1,), (1,)), ((), ())), preferred_element_type=F32)
    queries = (both[:D] * QUERY_SCALE).astype(BF)
    values = both[D:].astype(BF)
    keys = dot(normed, wk).astype(BF)
    ones = jnp.ones((16, LENGTH), BF)
    heads = []
    for h in range(HEADS):
        rows = slice(h * HEAD, (h + 1) * HEAD)
        scores = dot(keys[:, rows], queries[rows])
        top = jnp.max(scores, axis=0, keepdims=True)
        weights = jnp.exp2(scores - top).astype(BF)
        summed = dot(jnp.concatenate([values[rows], ones], axis=0), weights)
        heads.append((summed[:HEAD] * (1.0 / summed[HEAD : HEAD + 1])).astype(BF))
    attended = jnp.concatenate(heads, axis=0).T
    after = state + dot(attended, wo)
    normed = layer_norm(after, gains[1:2], biases[1:2]).astype(BF)
    out = after
    for c in range(4):
        hidden = slice(c * 256, (c + 1) * 256)
        active = jnp.maximum(dot(normed, up[:, hidden]), 0.0).astype(BF)
        out = out + dot(active, down[hidden])
    return out


def combine(total, spread, count, cells):
    whole = jnp.sum(total, axis=0, keepdims=True)
    offset = total - whole * (1.0 / count)
    square = jnp.sum(spread, axis=0, keepdims=True)
    return whole, square + jnp.sum(offset * offset, axis=0, keepdims=True) * (1.0 / cells)


def pack_stats(total, spread):
    row = lax.broadcasted_iota(jnp.int32, (8, 128), 0)
    wide_total = jnp.broadcast_to(total, (8, 128))
    return jnp.where(row == 0, wide_total, jnp.broadcast_to(spread, (8, 128)))


def kernel(
    mix_ref, attn_ref, up_ref, down_ref, gain_ref, bias_ref, ggain_ref, gbias_ref, pos_ref,
    out_ref,
    state, qv_t, y, carried, plane_in, column_out, inter, column_in, plane_out, back, flat,
    half, stat_own, stat_a, stat_mid, stat_b, sent, recv, load_sem,
):
    index = lax.axis_index("wide") * 16 + lax.axis_index("narrow")
    plane = lax.div(index, 8)
    column = lax.rem(index, 8)

    def device(p, r):
        return (lax.div(p, 2), lax.rem(p, 2) * 8 + r)

    def each_column(work):
        def one(k, _):
            work(lax.rem(column + k, COLUMN))
            return 0

        lax.fori_loop(1, COLUMN, one, 0)

    def each_plane(work):
        def one(k, _):
            work(lax.rem(plane + k, PLANE))
            return 0

        lax.fori_loop(1, PLANE, one, 0)

    def remote(src, dst, kind, slot, p, r):
        return pltpu.make_async_remote_copy(
            src_ref=src, dst_ref=dst, send_sem=sent.at[kind, slot], recv_sem=recv.at[kind, slot],
            device_id=device(p, r), device_id_type=MESH,
        )

    def arrived(ref, kind, slot):
        pltpu.make_async_copy(ref, ref, recv.at[kind, slot]).wait()

    def left(ref, kind, slot):
        pltpu.make_async_copy(ref, ref, sent.at[kind, slot]).wait()

    load = pltpu.make_async_copy(mix_ref, state.at[0], load_sem)
    load.start()

    barrier = pltpu.get_barrier_semaphore()
    each_column(
        lambda r: pl.semaphore_signal(
            barrier, inc=1, device_id=device(plane, r), device_id_type=MESH
        )
    )
    each_plane(
        lambda p: pl.semaphore_signal(
            barrier, inc=1, device_id=device(p, column), device_id_type=MESH
        )
    )
    pl.semaphore_wait(barrier, COLUMN - 1 + PLANE - 1)

    for l in range(2):
        for i, j in ((0, 0), (1, 2)):
            qv_t[l, i * D : (i + 1) * D] = attn_ref[l, j].T

    load.wait()

    def compute(t):
        l = lax.div(t, 8)
        b = lax.div(lax.rem(t, 8), 2)
        s = lax.rem(t, 2)
        start = state[l, b, s].astype(F32) + pos_ref[l]
        out = encoder(
            start, gain_ref[l], bias_ref[l], qv_t[l], attn_ref[l, 1], attn_ref[l, 3],
            up_ref.at[l], down_ref.at[l],
        )
        y[b, s] = out

        @pl.when(l == 1)
        def _():
            rounded = out.astype(BF)
            inter[b, s] = rounded
            y[b, s] = rounded.astype(F32)
            each_column(
                lambda r: remote(
                    inter.at[b, s, pl.ds(pl.multiple_of(r * 32, 32), 32)],
                    column_in.at[b, 2 * column + s],
                    4, b, plane, r,
                ).start()
            )
            mine = pl.ds(pl.multiple_of(column * 32, 32), 32)
            column_in[b, 2 * column + s] = inter[b, s, mine]

        done = y[b, s]
        total = jnp.sum(jnp.sum(done, axis=0, keepdims=True), axis=1, keepdims=True)
        offset = done - total * (1.0 / SEQ_CELLS)
        spread = jnp.sum(jnp.sum(offset * offset, axis=0, keepdims=True), axis=1, keepdims=True)
        half[s] = pack_stats(total, spread)

    def start_stats(slot):
        total, spread = combine(half[:, 0, :], half[:, 1, :], 2, SEQ_CELLS)
        packed = pack_stats(total, spread)
        stat_own[slot] = packed
        stat_a[slot, column] = packed
        each_column(
            lambda r: remote(
                stat_own.at[slot], stat_a.at[slot, column], 0, slot, plane, r
            ).start()
        )

    def relay_stats(slot):
        arrived(stat_a.at[slot, pl.ds(0, COLUMN - 1)], 0, slot)
        total, spread = combine(stat_a[slot, :, 0, :], stat_a[slot, :, 1, :], COLUMN, UNIT_CELLS)
        packed = pack_stats(total, spread)
        stat_mid[slot] = packed
        stat_b[slot, plane] = packed
        each_plane(
            lambda p: remote(
                stat_mid.at[slot], stat_b.at[slot, plane], 1, slot, p, column
            ).start()
        )

    def mixture_stats(slot):
        arrived(stat_b.at[slot, pl.ds(0, PLANE - 1)], 1, slot)
        total, spread = combine(stat_b[slot, :, 0, :], stat_b[slot, :, 1, :], PLANE, COLUMN_CELLS)
        mean = total * (1.0 / MIX_CELLS)
        scale = lax.rsqrt(spread * (1.0 / MIX_CELLS) + EPSILON)
        return (
            jnp.concatenate([mean, mean], axis=1),
            jnp.concatenate([scale, scale], axis=1),
        )

    def carry(b):
        mean, scale = mixture_stats(b)
        for s in range(2):
            normed = (y[b, s] - mean) * scale * ggain_ref[0:1] + gbias_ref[0:1]
            carried[b, s] = (normed + state[0, b, s].astype(F32)).astype(BF)
        mine = pl.ds(pl.multiple_of(plane * 16, 16), 16)
        plane_in[b, plane] = carried[b, :, mine, :]
        each_plane(
            lambda p: remote(
                carried.at[b, :, pl.ds(pl.multiple_of(p * 16, 16), 16), :],
                plane_in.at[b, plane],
                2, b, p, column,
            ).start()
        )

    def regroup(b):
        arrived(plane_in.at[b, pl.ds(0, PLANE - 1)], 2, b)
        for c in range(2):
            lanes = slice(c * 128, (c + 1) * 128)
            flat[c] = plane_in[b, :, :, :, lanes].reshape(512, 128).astype(F32)
            for f in range(16):
                column_out[b, f, :, lanes] = flat[c, pl.ds(f, 32, stride=16), :].astype(BF)
        mine = pl.ds(pl.multiple_of(column * 32, 32), 32)
        state[1, b, :, mine, :] = column_out[b, pl.ds(2 * column, 2)]
        each_column(
            lambda r: remote(
                column_out.at[b, pl.ds(2 * r, 2)], state.at[1, b, :, mine, :], 3, b, plane, r
            ).start()
        )

    def regroup_back(b):
        arrived(column_in.at[b, pl.ds(0, 2 * (COLUMN - 1))], 4, b)
        for c in range(2):
            lanes = slice(c * 128, (c + 1) * 128)
            flat[c] = column_in[b, :, :, lanes].reshape(512, 128).astype(F32)
            for q in range(32):
                plane_out[b, q, :, lanes] = flat[c, pl.ds(q, 16, stride=32), :].astype(BF)
        mine = pl.ds(pl.multiple_of(plane * 16, 16), 16)
        back[b, :, mine, :] = plane_out[b, pl.ds(2 * plane, 2)]
        each_plane(
            lambda p: remote(
                plane_out.at[b, pl.ds(2 * p, 2)], back.at[b, :, mine, :], 5, b, p, column
            ).start()
        )

    def finish(b):
        mean, scale = mixture_stats(4 + b)
        arrived(back.at[b, :, pl.ds(0, 16 * (PLANE - 1)), :], 5, b)
        for s in range(2):
            normed = (back[b, s].astype(F32) - mean) * scale * ggain_ref[1:2] + gbias_ref[1:2]
            out_ref[b, s] = (normed + carried[b, s].astype(F32)).astype(BF)

    def step(t, _):
        def when(first, last, parity, work):
            due = (t >= first) & (t <= last) & (lax.rem(t, 2) == parity)
            pl.when(due)(lambda: work(lax.div(t - first, 2)))

        @pl.when((t >= 8) & (t < 16) & (lax.rem(t, 2) == 0))
        def _():
            b = lax.div(t - 8, 2)
            arrived(state.at[1, b, :, pl.ds(0, 32 * (COLUMN - 1)), :], 3, b)

        @pl.when(t < 16)
        def _():
            compute(t)

        when(1, 15, 1, start_stats)
        when(2, 16, 0, relay_stats)
        when(3, 9, 1, carry)
        when(5, 11, 1, regroup)
        when(11, 17, 1, regroup_back)
        when(13, 19, 1, finish)
        return 0

    lax.fori_loop(0, 20, step, 0)

    def drain(b, _):
        for slot in (b, 4 + b):
            left(stat_a.at[slot, pl.ds(0, COLUMN - 1)], 0, slot)
            left(stat_b.at[slot, pl.ds(0, PLANE - 1)], 1, slot)
        left(plane_in.at[b, pl.ds(0, PLANE - 1)], 2, b)
        left(state.at[1, b, :, pl.ds(0, 32 * (COLUMN - 1)), :], 3, b)
        left(column_in.at[b, pl.ds(0, 2 * (COLUMN - 1))], 4, b)
        left(back.at[b, :, pl.ds(0, 16 * (PLANE - 1)), :], 5, b)
        return 0

    lax.fori_loop(0, MIX, drain, 0)


def on_device(mixture, w_attn, w_up, w_down, norm_gain, norm_bias, group_gain, group_bias):
    vmem = pl.BlockSpec(memory_space=pltpu.VMEM)
    return pl.pallas_call(
        kernel,
        name="dual_path",
        out_shape=jax.ShapeDtypeStruct(mixture.shape, BF),
        in_specs=[pl.BlockSpec(memory_space=pl.ANY)] + [vmem] * 8,
        out_specs=vmem,
        scratch_shapes=[
            pltpu.VMEM((2, MIX, 2, LENGTH, D), BF),
            pltpu.VMEM((2, 2 * D, D), BF),
            pltpu.VMEM((MIX, 2, LENGTH, D), F32),
            pltpu.VMEM((MIX, 2, LENGTH, D), BF),
            pltpu.VMEM((MIX, PLANE, 2, 16, D), BF),
            pltpu.VMEM((MIX, 16, 32, D), BF),
            pltpu.VMEM((MIX, 2, LENGTH, D), BF),
            pltpu.VMEM((MIX, 16, 32, D), BF),
            pltpu.VMEM((MIX, 32, 16, D), BF),
            pltpu.VMEM((MIX, 2, LENGTH, D), BF),
            pltpu.VMEM((2, 512, 128), F32),
            pltpu.VMEM((2, 8, 128), F32),
            pltpu.VMEM((8, 8, 128), F32),
            pltpu.VMEM((8, COLUMN, 8, 128), F32),
            pltpu.VMEM((8, 8, 128), F32),
            pltpu.VMEM((8, PLANE, 8, 128), F32),
            pltpu.SemaphoreType.DMA((6, 8)),
            pltpu.SemaphoreType.DMA((6, 8)),
            pltpu.SemaphoreType.DMA,
        ],
        compiler_params=pltpu.CompilerParams(
            collective_id=0, has_side_effects=True, vmem_limit_bytes=48 * 1024 * 1024
        ),
    )(
        mixture, w_attn, w_up, w_down, norm_gain, norm_bias, group_gain, group_bias,
        jnp.asarray(position_tables()),
    )


def solution(mesh):
    split = P(None, ("wide", "narrow"), None, None)
    return jax.shard_map(
        on_device, mesh=mesh, in_specs=(split,) + (P(),) * 7, out_specs=split, check_vma=False
    )
```

```python
import math

import jax
import jax.numpy as jnp
import numpy as np
from jax import lax
from jax.experimental import pallas as pl
from jax.experimental.pallas import tpu as pltpu
from jax.sharding import PartitionSpec as P

F32 = jnp.float32
BF = jnp.bfloat16
MESH = pl.DeviceIdType.MESH

HEADS = 8
HEAD = 32
D = 256
LENGTH = 256
MIX = 4
PLANE = 16
COLUMN = 8
CHIPS = 64
EPSILON = 1e-05
QUERY_SCALE = math.log2(math.e) / math.sqrt(HEAD)
UNIT_CELLS = 2.0 * LENGTH * D
COLUMN_CELLS = UNIT_CELLS * COLUMN
MIX_CELLS = COLUMN_CELLS * PLANE
FAR_FIRST = sorted(
    range(1, CHIPS), key=lambda k: -sum((0, 1, 2, 1)[k // d % 4] for d in (1, 4, 16))
)
S2_AT = 3
V_AT = 14
N_AT = 7
R_AT = 8
RR_AT = 20
F_AT = 22


def position_tables():
    positions = np.arange(LENGTH, dtype=np.float32)[:, None]
    freq = np.arange(D // 2, dtype=np.float32)[None, :]
    angles = positions * np.exp(freq * np.float32(-2.0 * math.log(10000.0) / D))
    table = np.concatenate([np.sin(angles), np.cos(angles)], axis=1).astype(np.float32)
    s, chip = np.meshgrid(np.arange(4), np.arange(CHIPS), indexing="ij")
    order = (4 * chip + s).reshape(-1)
    return np.stack([table, table[order]])


def dot(a, b):
    return jnp.dot(a, b, preferred_element_type=F32)


def layer_norm(rows, gain, bias):
    mean = jnp.mean(rows, axis=-1, keepdims=True)
    centered = rows - mean
    variance = jnp.mean(centered * centered, axis=-1, keepdims=True)
    return centered * lax.rsqrt(variance + EPSILON) * gain + bias


def attention(states, gain, bias, qv_t, wk, wo):
    normed = [layer_norm(state, gain, bias).astype(BF) for state in states]
    both = [
        lax.dot_general(qv_t, rows, (((1,), (1,)), ((), ())), preferred_element_type=F32)
        for rows in normed
    ]
    queries = [(part[:D] * QUERY_SCALE).astype(BF) for part in both]
    values = [part[D:].astype(BF) for part in both]
    keys = [dot(rows, wk).astype(BF) for rows in normed]
    ones = jnp.ones((16, LENGTH), BF)
    after = []
    for state, query, key, value in zip(states, queries, keys, values):
        rows = [slice(h * HEAD, (h + 1) * HEAD) for h in range(HEADS)]
        scores = [dot(key[:, r], query[r]) for r in rows]
        weights = [
            jnp.exp2(part - jnp.max(part, axis=0, keepdims=True)).astype(BF) for part in scores
        ]
        summed = [
            dot(jnp.concatenate([value[r], ones], axis=0), part) for r, part in zip(rows, weights)
        ]
        heads = [(part[:HEAD] * (1.0 / part[HEAD : HEAD + 1])).astype(BF) for part in summed]
        after.append(jnp.concatenate(heads, axis=0).T)
    return [state + dot(rows, wo) for state, rows in zip(states, after)]


def feed_forward(afters, gain, bias, up, down):
    normed = [layer_norm(after, gain, bias).astype(BF) for after in afters]
    active = [jnp.maximum(dot(rows, up), 0.0).astype(BF) for rows in normed]
    return [after + dot(rows, down) for after, rows in zip(afters, active)]


def combine(total, spread, count, cells):
    whole = jnp.sum(total, axis=0, keepdims=True)
    offset = total - whole * (1.0 / count)
    square = jnp.sum(spread, axis=0, keepdims=True)
    return whole, square + jnp.sum(offset * offset, axis=0, keepdims=True) * (1.0 / cells)


def pack_stats(total, spread):
    row = lax.broadcasted_iota(jnp.int32, (8, 128), 0)
    wide_total = jnp.broadcast_to(total, (8, 128))
    return jnp.where(row == 0, wide_total, jnp.broadcast_to(spread, (8, 128)))


def kernel(
    mix_ref, attn_hbm, up_hbm, down_hbm, gain_hbm, bias_hbm, ggain_hbm, gbias_hbm, pos_hbm,
    out_ref,
    attn_ref, up_ref, down_ref, gain_ref, bias_ref, ggain_ref, gbias_ref, pos_ref,
    state, qv_t, middle, y, carried, pair_in, chip_out, chip_in, back_out, back_in, pair_out,
    back, flat, partial, stat_own, stat_a, stat_mid, stat_b, sent, recv, load_sem,
):
    index = lax.axis_index("wide") * 16 + lax.axis_index("narrow")
    plane = lax.div(index, 8)
    column = lax.rem(index, 8)
    chip = lax.div(index, 2)
    core = lax.rem(index, 2)
    partner = column + 1 - 2 * core
    half = pl.ds(pl.multiple_of(core * 128, 128), 128)
    other_half = pl.ds(pl.multiple_of(128 - core * 128, 128), 128)

    def device(p, r):
        return (lax.div(p, 2), lax.rem(p, 2) * 8 + r)

    def each_column(work):
        for k in range(1, COLUMN):
            work(lax.rem(column + k, COLUMN))

    def each_plane(work):
        for k in range(1, PLANE):
            work(lax.rem(plane + k, PLANE))

    def each_chip(work):
        for k in FAR_FIRST:
            x = lax.rem(lax.div(chip, 16) + k // 16, 4)
            y_ = lax.rem(lax.div(lax.rem(chip, 16), 4) + k // 4 % 4, 4)
            z = lax.rem(lax.rem(chip, 4) + k % 4, 4)
            work(x, y_, z)

    def chip_device(x, y_, z, c):
        return (x * 2 + lax.div(y_, 2), lax.rem(y_, 2) * 8 + z * 2 + c)

    def remote(src, dst, kind, slot, where):
        return pltpu.make_async_remote_copy(
            src_ref=src, dst_ref=dst, send_sem=sent.at[kind, slot], recv_sem=recv.at[kind, slot],
            device_id=where, device_id_type=MESH,
        )

    def arrived(ref, kind, slot):
        pltpu.make_async_copy(ref, ref, recv.at[kind, slot]).wait()

    def left(ref, kind, slot):
        pltpu.make_async_copy(ref, ref, sent.at[kind, slot]).wait()

    loads = (
        ((mix_ref.at[0], state.at[0]), (attn_hbm.at[0], attn_ref.at[0]),
         (gain_hbm, gain_ref), (bias_hbm, bias_ref), (pos_hbm.at[0], pos_ref.at[0])),
        ((up_hbm.at[0], up_ref.at[0]), (down_hbm.at[0], down_ref.at[0])),
        ((mix_ref.at[pl.ds(1, MIX - 1)], state.at[pl.ds(1, MIX - 1)]),
         (ggain_hbm, ggain_ref), (gbias_hbm, gbias_ref)),
        ((attn_hbm.at[1], attn_ref.at[1]), (pos_hbm.at[1], pos_ref.at[1]),
         (up_hbm.at[1], up_ref.at[1]), (down_hbm.at[1], down_ref.at[1])),
    )
    loads = [
        [pltpu.make_async_copy(src, dst, load_sem.at[i, j]) for j, (src, dst) in enumerate(group)]
        for i, group in enumerate(loads)
    ]
    for group in loads:
        for copy in group:
            copy.start()

    def loaded(i):
        for copy in loads[i]:
            copy.wait()

    barrier = pltpu.get_barrier_semaphore()

    def greet(where):
        pl.semaphore_signal(barrier, inc=1, device_id=where, device_id_type=MESH)

    each_chip(lambda x, y_, z: greet(chip_device(x, y_, z, core)))
    for z in range(4):
        greet(device(plane, z * 2 + (1 - core)))

    def turn(l):
        for i, j in ((0, 0), (1, 2)):
            qv_t[l, i * D : (i + 1) * D] = attn_ref[l, j].T

    def first_half(t):
        l = lax.div(t, 8)
        b = lax.div(lax.rem(t, 8), 2)

        @pl.when(l == 0)
        def _():
            for s in range(2):
                middle[s] = state[b, s].astype(F32)

        @pl.when(l == 1)
        def _():
            arrived(chip_in.at[b, pl.ds(0, CHIPS - 1)], 3, b)
            for c in range(2):
                lanes = slice(c * 128, (c + 1) * 128)
                flat[c] = chip_in[b, :, :, lanes].reshape(512, 128).astype(F32)
                for f in range(2):
                    for s in range(4):
                        middle[f, s * CHIPS : (s + 1) * CHIPS, lanes] = flat[
                            c, pl.ds(4 * f + s, CHIPS, stride=8), :
                        ]

        starts = [middle[s] + pos_ref[l] for s in range(2)]
        after = attention(
            starts, gain_ref[l, 0:1], bias_ref[l, 0:1], qv_t[l], attn_ref[l, 1], attn_ref[l, 3]
        )
        for s in range(2):
            middle[s] = after[s]

    def second_half(t):
        l = lax.div(t, 8)
        b = lax.div(lax.rem(t, 8), 2)
        afters = [middle[s] for s in range(2)]
        outs = feed_forward(
            afters, gain_ref[l, 1:2], bias_ref[l, 1:2], up_ref[l], down_ref[l]
        )
        pivot = None
        for s in range(2):
            out = jnp.where(l == 0, outs[s], outs[s].astype(BF).astype(F32))
            y[b, s] = out
            if pivot is None:
                pivot = out[:8]
                near = square = jnp.zeros((8, D), F32)
            offset = out.reshape(LENGTH // 8, 8, D) - pivot[None]
            near = near + jnp.sum(offset, axis=0)
            square = square + jnp.sum(offset * offset, axis=0)
        partial[0] = pivot
        partial[1] = near
        partial[2] = square

    def send_back(b):
        for c in range(2):
            lanes = slice(c * 128, (c + 1) * 128)
            for f in range(2):
                for s in range(4):
                    flat[c, pl.ds(4 * f + s, CHIPS, stride=8), :] = y[
                        b, f, s * CHIPS : (s + 1) * CHIPS, lanes
                    ]
            back_out[b, :, :, lanes] = flat[c].reshape(CHIPS, 8, 128).astype(BF)
        back_in[b, chip] = back_out[b, chip]
        each_chip(
            lambda x, y_, z: remote(
                back_out.at[b, x * 16 + y_ * 4 + z], back_in.at[b, chip],
                4, b, chip_device(x, y_, z, core),
            ).start()
        )

    def start_stats(slot):
        near = partial[1]
        totals = near + partial[0] * 64.0
        spreads = partial[2] - near * near * (1.0 / 64.0)
        whole = jnp.sum(jnp.sum(totals, axis=0, keepdims=True), axis=1, keepdims=True)
        offset = totals - whole * (1.0 / 2048.0)
        spreads = spreads + offset * offset * (1.0 / 64.0)
        spread = jnp.sum(jnp.sum(spreads, axis=0, keepdims=True), axis=1, keepdims=True)
        packed = pack_stats(whole, spread)
        stat_own[slot] = packed
        stat_a[slot, column] = packed
        each_column(
            lambda r: remote(
                stat_own.at[slot], stat_a.at[slot, column], 0, slot, device(plane, r)
            ).start()
        )

    def relay_stats(slot):
        arrived(stat_a.at[slot, pl.ds(0, COLUMN - 1)], 0, slot)
        total, spread = combine(stat_a[slot, :, 0, :], stat_a[slot, :, 1, :], COLUMN, UNIT_CELLS)
        packed = pack_stats(total, spread)
        stat_mid[slot] = packed
        stat_b[slot, plane] = packed
        each_plane(
            lambda p: remote(
                stat_mid.at[slot], stat_b.at[slot, plane], 1, slot, device(p, column)
            ).start()
        )

    def mixture_stats(slot):
        arrived(stat_b.at[slot, pl.ds(0, PLANE - 1)], 1, slot)
        total, spread = combine(stat_b[slot, :, 0, :], stat_b[slot, :, 1, :], PLANE, COLUMN_CELLS)
        mean = total * (1.0 / MIX_CELLS)
        scale = lax.rsqrt(spread * (1.0 / MIX_CELLS) + EPSILON)
        return (
            jnp.concatenate([mean, mean], axis=1),
            jnp.concatenate([scale, scale], axis=1),
        )

    def carry(b):
        mean, scale = mixture_stats(b)
        for s in range(2):
            normed = (y[b, s] - mean) * scale * ggain_ref[0:1] + gbias_ref[0:1]
            carried[b, s] = (normed + state[b, s].astype(F32)).astype(BF)
        remote(
            carried.at[b, :, other_half, :], pair_in.at[b, core], 2, b, device(plane, partner)
        ).start()
        pair_in[b, core] = carried[b, :, half, :]

    def regroup(b):
        arrived(pair_in.at[b, 0], 2, b)
        for c in range(2):
            lanes = slice(c * 128, (c + 1) * 128)
            for s in range(4):
                flat[c, pl.ds(s, 128, stride=4), :] = pair_in[b, s // 2, s % 2, :, lanes].astype(
                    F32
                )
            chip_out[b, :, :, lanes] = flat[c].reshape(CHIPS, 8, 128).astype(BF)
        chip_in[b, chip] = chip_out[b, chip]
        each_chip(
            lambda x, y_, z: remote(
                chip_out.at[b, x * 16 + y_ * 4 + z], chip_in.at[b, chip],
                3, b, chip_device(x, y_, z, core),
            ).start()
        )

    def regroup_back(b):
        arrived(back_in.at[b, pl.ds(0, CHIPS - 1)], 4, b)
        for c in range(2):
            lanes = slice(c * 128, (c + 1) * 128)
            flat[c] = back_in[b, :, :, lanes].reshape(512, 128).astype(F32)
            for s in range(4):
                pair_out[b, s // 2, s % 2, :, lanes] = flat[c, pl.ds(s, 128, stride=4), :].astype(
                    BF
                )
        remote(
            pair_out.at[b, 1 - core], back.at[b, :, half, :], 5, b, device(plane, partner)
        ).start()
        back[b, :, half, :] = pair_out[b, core]

    def finish(b):
        mean, scale = mixture_stats(4 + b)
        arrived(back.at[b, :, pl.ds(0, 128), :], 5, b)
        for s in range(2):
            normed = (back[b, s].astype(F32) - mean) * scale * ggain_ref[1:2] + gbias_ref[1:2]
            out_ref[b, s] = (normed + carried[b, s].astype(F32)).astype(BF)

    def step(t, _):
        def when(first, work, count=4):
            due = (t >= first) & (t <= first + 2 * count - 2) & (lax.rem(t, 2) == first % 2)
            pl.when(due)(lambda: work(lax.div(t - first, 2)))

        pl.when(t == 1)(lambda: loaded(1))
        pl.when(t == 2)(lambda: loaded(2))

        @pl.when(t == 8)
        def _():
            loaded(3)
            turn(1)

        pl.when(t == 1)(lambda: pl.semaphore_wait(barrier, CHIPS - 1 + 4))
        unit = jnp.where(t < 8, t, t - (V_AT - 8))
        busy = (t < 8) | ((t >= V_AT) & (t < V_AT + 8))
        pl.when(busy & (lax.rem(t, 2) == 0))(lambda: first_half(unit))

        @pl.when(busy & (lax.rem(t, 2) == 1))
        def _():
            second_half(unit)
            start_stats(lax.div(unit, 2))
            pl.when(t >= V_AT)(lambda: send_back(lax.div(unit - 8, 2)))

        when(S2_AT, relay_stats)
        when(V_AT + S2_AT, lambda b: relay_stats(4 + b))
        when(N_AT, carry)
        when(R_AT, regroup)
        when(RR_AT, regroup_back)
        when(F_AT, finish)
        return 0

    loaded(0)
    turn(0)
    lax.fori_loop(0, F_AT + 7, step, 0)

    def drain(b, _):
        for slot in (b, 4 + b):
            left(stat_a.at[slot, pl.ds(0, COLUMN - 1)], 0, slot)
            left(stat_b.at[slot, pl.ds(0, PLANE - 1)], 1, slot)
        left(pair_in.at[b, 0], 2, b)
        left(chip_in.at[b, pl.ds(0, CHIPS - 1)], 3, b)
        left(back_in.at[b, pl.ds(0, CHIPS - 1)], 4, b)
        left(pair_out.at[b, 0], 5, b)
        return 0

    lax.fori_loop(0, MIX, drain, 0)


def on_device(mixture, w_attn, w_up, w_down, norm_gain, norm_bias, group_gain, group_bias):
    hbm = pl.BlockSpec(memory_space=pltpu.HBM)
    return pl.pallas_call(
        kernel,
        name="dual_path",
        out_shape=jax.ShapeDtypeStruct(mixture.shape, BF),
        in_specs=[hbm] * 9,
        out_specs=pl.BlockSpec(memory_space=pltpu.VMEM),
        scratch_shapes=[
            pltpu.VMEM((2, 4, D, D), BF),
            pltpu.VMEM((2, D, 4 * D), BF),
            pltpu.VMEM((2, 4 * D, D), BF),
            pltpu.VMEM((2, 2, D), F32),
            pltpu.VMEM((2, 2, D), F32),
            pltpu.VMEM((2, D), F32),
            pltpu.VMEM((2, D), F32),
            pltpu.VMEM((2, LENGTH, D), F32),
            pltpu.VMEM((MIX, 2, LENGTH, D), BF),
            pltpu.VMEM((2, 2 * D, D), BF),
            pltpu.VMEM((2, LENGTH, D), F32),
            pltpu.VMEM((MIX, 2, LENGTH, D), F32),
            pltpu.VMEM((MIX, 2, LENGTH, D), BF),
            pltpu.VMEM((MIX, 2, 2, 128, D), BF),
            pltpu.VMEM((MIX, CHIPS, 8, D), BF),
            pltpu.VMEM((MIX, CHIPS, 8, D), BF),
            pltpu.VMEM((MIX, CHIPS, 8, D), BF),
            pltpu.VMEM((MIX, CHIPS, 8, D), BF),
            pltpu.VMEM((MIX, 2, 2, 128, D), BF),
            pltpu.VMEM((MIX, 2, LENGTH, D), BF),
            pltpu.VMEM((2, 512, 128), F32),
            pltpu.VMEM((3, 8, D), F32),
            pltpu.VMEM((8, 8, 128), F32),
            pltpu.VMEM((8, COLUMN, 8, 128), F32),
            pltpu.VMEM((8, 8, 128), F32),
            pltpu.VMEM((8, PLANE, 8, 128), F32),
            pltpu.SemaphoreType.DMA((6, 8)),
            pltpu.SemaphoreType.DMA((6, 8)),
            pltpu.SemaphoreType.DMA((4, 5)),
        ],
        compiler_params=pltpu.CompilerParams(
            collective_id=0, has_side_effects=True, vmem_limit_bytes=60 * 1024 * 1024
        ),
    )(
        mixture, w_attn, w_up, w_down, norm_gain, norm_bias, group_gain, group_bias,
        jnp.asarray(position_tables()),
    )


def solution(mesh):
    split = P(None, ("wide", "narrow"), None, None)
    return jax.shard_map(
        on_device, mesh=mesh, in_specs=(split,) + (P(),) * 7, out_specs=split, check_vma=False
    )
```

```python
import math

import jax
import jax.numpy as jnp
import numpy as np
from jax import lax
from jax.experimental import pallas as pl
from jax.experimental.pallas import tpu as pltpu
from jax.sharding import PartitionSpec as P

F32 = jnp.float32
BF = jnp.bfloat16
MESH = pl.DeviceIdType.MESH

HEADS = 8
HEAD = 32
D = 256
LENGTH = 256
MIX = 4
PLANE = 16
COLUMN = 8
CHIPS = 64
EPSILON = 1e-05
QUERY_SCALE = math.log2(math.e) / math.sqrt(HEAD)
UNIT_CELLS = 2.0 * LENGTH * D
COLUMN_CELLS = UNIT_CELLS * COLUMN
MIX_CELLS = COLUMN_CELLS * PLANE
FAR_FIRST = sorted(
    range(1, CHIPS), key=lambda k: -sum((0, 1, 2, 1)[k // d % 4] for d in (1, 4, 16))
)
S2_AT = 4
V_AT = 14
N_AT = 7
R_AT = 8
RR_AT = 20
F_AT = 22
S2V_AT = 18


def position_tables():
    positions = np.arange(LENGTH, dtype=np.float32)[:, None]
    freq = np.arange(D // 2, dtype=np.float32)[None, :]
    angles = positions * np.exp(freq * np.float32(-2.0 * math.log(10000.0) / D))
    table = np.concatenate([np.sin(angles), np.cos(angles)], axis=1).astype(np.float32)
    s, chip = np.meshgrid(np.arange(4), np.arange(CHIPS), indexing="ij")
    order = (4 * chip + s).reshape(-1)
    return np.stack([table, table[order]])


def dot(a, b):
    return jnp.dot(a, b, preferred_element_type=F32)


def layer_norm(rows, gain, bias):
    mean = jnp.mean(rows, axis=-1, keepdims=True)
    centered = rows - mean
    variance = jnp.mean(centered * centered, axis=-1, keepdims=True)
    return centered * lax.rsqrt(variance + EPSILON) * gain + bias


def attention(states, gain, bias, qv_t, wk, wo):
    normed = [layer_norm(state, gain, bias).astype(BF) for state in states]
    both = [
        lax.dot_general(qv_t, rows, (((1,), (1,)), ((), ())), preferred_element_type=F32)
        for rows in normed
    ]
    queries = [(part[:D] * QUERY_SCALE).astype(BF) for part in both]
    values = [part[D:].astype(BF) for part in both]
    keys = [dot(rows, wk).astype(BF) for rows in normed]
    ones = jnp.ones((16, LENGTH), BF)
    after = []
    for state, query, key, value in zip(states, queries, keys, values):
        rows = [slice(h * HEAD, (h + 1) * HEAD) for h in range(HEADS)]
        scores = [dot(key[:, r], query[r]) for r in rows]
        weights = [
            jnp.exp2(part - jnp.max(part, axis=0, keepdims=True)).astype(BF) for part in scores
        ]
        summed = [
            dot(jnp.concatenate([value[r], ones], axis=0), part) for r, part in zip(rows, weights)
        ]
        heads = [(part[:HEAD] * (1.0 / part[HEAD : HEAD + 1])).astype(BF) for part in summed]
        after.append(jnp.concatenate(heads, axis=0).T)
    return [state + dot(rows, wo) for state, rows in zip(states, after)]


def feed_forward(afters, gain, bias, up, down):
    normed = [layer_norm(after, gain, bias).astype(BF) for after in afters]
    active = [jnp.maximum(dot(rows, up), 0.0).astype(BF) for rows in normed]
    return [after + dot(rows, down) for after, rows in zip(afters, active)]


def combine(total, spread, count, cells):
    whole = jnp.sum(total, axis=0, keepdims=True)
    offset = total - whole * (1.0 / count)
    square = jnp.sum(spread, axis=0, keepdims=True)
    return whole, square + jnp.sum(offset * offset, axis=0, keepdims=True) * (1.0 / cells)


def pack_stats(total, spread):
    row = lax.broadcasted_iota(jnp.int32, (8, 128), 0)
    wide_total = jnp.broadcast_to(total, (8, 128))
    return jnp.where(row == 0, wide_total, jnp.broadcast_to(spread, (8, 128)))


def kernel(
    mix_ref, attn_hbm, up_hbm, down_hbm, gain_hbm, bias_hbm, ggain_hbm, gbias_hbm, pos_hbm,
    out_ref,
    attn_ref, up_ref, down_ref, gain_ref, bias_ref, ggain_ref, gbias_ref, pos_ref,
    state, qv_t, middle, y, carried, pair_in, chip_out, chip_in, back_out, back_in, pair_out,
    back, flat, partial, stat_own, stat_a, stat_mid, stat_b, sent, recv, load_sem,
):
    index = lax.axis_index("wide") * 16 + lax.axis_index("narrow")
    plane = lax.div(index, 8)
    column = lax.rem(index, 8)
    chip = lax.div(index, 2)
    core = lax.rem(index, 2)
    partner = column + 1 - 2 * core
    half = pl.ds(pl.multiple_of(core * 128, 128), 128)
    other_half = pl.ds(pl.multiple_of(128 - core * 128, 128), 128)

    def device(p, r):
        return (lax.div(p, 2), lax.rem(p, 2) * 8 + r)

    def each_column(work):
        for k in range(1, COLUMN):
            work(lax.rem(column + k, COLUMN))

    def each_plane(work):
        for k in range(1, PLANE):
            work(lax.rem(plane + k, PLANE))

    def each_chip(work):
        for k in FAR_FIRST:
            x = lax.rem(lax.div(chip, 16) + k // 16, 4)
            y_ = lax.rem(lax.div(lax.rem(chip, 16), 4) + k // 4 % 4, 4)
            z = lax.rem(lax.rem(chip, 4) + k % 4, 4)
            work(x, y_, z)

    def chip_device(x, y_, z, c):
        return (x * 2 + lax.div(y_, 2), lax.rem(y_, 2) * 8 + z * 2 + c)

    def remote(src, dst, kind, slot, where):
        return pltpu.make_async_remote_copy(
            src_ref=src, dst_ref=dst, send_sem=sent.at[kind, slot], recv_sem=recv.at[kind, slot],
            device_id=where, device_id_type=MESH,
        )

    def arrived(ref, kind, slot):
        pltpu.make_async_copy(ref, ref, recv.at[kind, slot]).wait()

    def left(ref, kind, slot):
        pltpu.make_async_copy(ref, ref, sent.at[kind, slot]).wait()

    loads = (
        ((mix_ref.at[0], state.at[0]), (attn_hbm.at[0], attn_ref.at[0]),
         (gain_hbm, gain_ref), (bias_hbm, bias_ref), (pos_hbm.at[0], pos_ref.at[0])),
        ((up_hbm.at[0], up_ref.at[0]), (down_hbm.at[0], down_ref.at[0])),
        ((mix_ref.at[pl.ds(1, MIX - 1)], state.at[pl.ds(1, MIX - 1)]),
         (ggain_hbm, ggain_ref), (gbias_hbm, gbias_ref)),
        ((attn_hbm.at[1], attn_ref.at[1]), (pos_hbm.at[1], pos_ref.at[1]),
         (up_hbm.at[1], up_ref.at[1]), (down_hbm.at[1], down_ref.at[1])),
    )
    loads = [
        [pltpu.make_async_copy(src, dst, load_sem.at[i, j]) for j, (src, dst) in enumerate(group)]
        for i, group in enumerate(loads)
    ]
    for group in loads:
        for copy in group:
            copy.start()

    def loaded(i):
        for copy in loads[i]:
            copy.wait()

    barrier = pltpu.get_barrier_semaphore()

    def greet(where):
        pl.semaphore_signal(barrier, inc=1, device_id=where, device_id_type=MESH)

    each_column(lambda r: greet(device(plane, r)))
    each_plane(lambda p: greet(device(p, column)))

    def turn(l):
        for i, j in ((0, 0), (1, 2)):
            qv_t[l, i * D : (i + 1) * D] = attn_ref[l, j].T

    def first_half(t):
        l = lax.div(t, 8)
        b = lax.div(lax.rem(t, 8), 2)

        @pl.when(l == 0)
        def _():
            for s in range(2):
                middle[s] = state[b, s].astype(F32)

        @pl.when(l == 1)
        def _():
            arrived(chip_in.at[b, pl.ds(0, CHIPS - 1)], 3, b)
            for c in range(2):
                lanes = slice(c * 128, (c + 1) * 128)
                flat[c] = chip_in[b, :, :, lanes].reshape(512, 128).astype(F32)
                for f in range(2):
                    for s in range(4):
                        middle[f, s * CHIPS : (s + 1) * CHIPS, lanes] = flat[
                            c, pl.ds(4 * f + s, CHIPS, stride=8), :
                        ]

        starts = [middle[s] + pos_ref[l] for s in range(2)]
        after = attention(
            starts, gain_ref[l, 0:1], bias_ref[l, 0:1], qv_t[l], attn_ref[l, 1], attn_ref[l, 3]
        )
        for s in range(2):
            middle[s] = after[s]

    def second_half(t):
        l = lax.div(t, 8)
        b = lax.div(lax.rem(t, 8), 2)
        afters = [middle[s] for s in range(2)]
        outs = feed_forward(
            afters, gain_ref[l, 1:2], bias_ref[l, 1:2], up_ref[l], down_ref[l]
        )
        pivot = None
        for s in range(2):
            out = jnp.where(l == 0, outs[s], outs[s].astype(BF).astype(F32))
            y[b, s] = out
            if pivot is None:
                pivot = out[:8]
                near = square = jnp.zeros((8, D), F32)
            offset = out.reshape(LENGTH // 8, 8, D) - pivot[None]
            near = near + jnp.sum(offset, axis=0)
            square = square + jnp.sum(offset * offset, axis=0)
        partial[0] = pivot
        partial[1] = near
        partial[2] = square

    def send_back(b):
        for c in range(2):
            lanes = slice(c * 128, (c + 1) * 128)
            for f in range(2):
                for s in range(4):
                    flat[c, pl.ds(4 * f + s, CHIPS, stride=8), :] = y[
                        b, f, s * CHIPS : (s + 1) * CHIPS, lanes
                    ]
            back_out[b, :, :, lanes] = flat[c].reshape(CHIPS, 8, 128).astype(BF)
        back_in[b, chip] = back_out[b, chip]
        each_chip(
            lambda x, y_, z: remote(
                back_out.at[b, x * 16 + y_ * 4 + z], back_in.at[b, chip],
                4, b, chip_device(x, y_, z, core),
            ).start()
        )

    def start_stats(slot):
        near = partial[1]
        totals = near + partial[0] * 64.0
        spreads = partial[2] - near * near * (1.0 / 64.0)
        whole = jnp.sum(jnp.sum(totals, axis=0, keepdims=True), axis=1, keepdims=True)
        offset = totals - whole * (1.0 / 2048.0)
        spreads = spreads + offset * offset * (1.0 / 64.0)
        spread = jnp.sum(jnp.sum(spreads, axis=0, keepdims=True), axis=1, keepdims=True)
        packed = pack_stats(whole, spread)
        stat_own[slot] = packed
        stat_a[slot, column] = packed
        each_column(
            lambda r: remote(
                stat_own.at[slot], stat_a.at[slot, column], 0, slot, device(plane, r)
            ).start()
        )

    def relay_stats(slot):
        arrived(stat_a.at[slot, pl.ds(0, COLUMN - 1)], 0, slot)
        total, spread = combine(stat_a[slot, :, 0, :], stat_a[slot, :, 1, :], COLUMN, UNIT_CELLS)
        packed = pack_stats(total, spread)
        stat_mid[slot] = packed
        stat_b[slot, plane] = packed
        each_plane(
            lambda p: remote(
                stat_mid.at[slot], stat_b.at[slot, plane], 1, slot, device(p, column)
            ).start()
        )

    def mixture_stats(slot):
        arrived(stat_b.at[slot, pl.ds(0, PLANE - 1)], 1, slot)
        total, spread = combine(stat_b[slot, :, 0, :], stat_b[slot, :, 1, :], PLANE, COLUMN_CELLS)
        mean = total * (1.0 / MIX_CELLS)
        scale = lax.rsqrt(spread * (1.0 / MIX_CELLS) + EPSILON)
        return (
            jnp.concatenate([mean, mean], axis=1),
            jnp.concatenate([scale, scale], axis=1),
        )

    def carry(b):
        mean, scale = mixture_stats(b)
        for s in range(2):
            normed = (y[b, s] - mean) * scale * ggain_ref[0:1] + gbias_ref[0:1]
            carried[b, s] = (normed + state[b, s].astype(F32)).astype(BF)
        remote(
            carried.at[b, :, other_half, :], pair_in.at[b, core], 2, b, device(plane, partner)
        ).start()
        pair_in[b, core] = carried[b, :, half, :]

    def regroup(b):
        arrived(pair_in.at[b, 0], 2, b)
        for c in range(2):
            lanes = slice(c * 128, (c + 1) * 128)
            for s in range(4):
                flat[c, pl.ds(s, 128, stride=4), :] = pair_in[b, s // 2, s % 2, :, lanes].astype(
                    F32
                )
            chip_out[b, :, :, lanes] = flat[c].reshape(CHIPS, 8, 128).astype(BF)
        chip_in[b, chip] = chip_out[b, chip]
        each_chip(
            lambda x, y_, z: remote(
                chip_out.at[b, x * 16 + y_ * 4 + z], chip_in.at[b, chip],
                3, b, chip_device(x, y_, z, core),
            ).start()
        )

    def regroup_back(b):
        arrived(back_in.at[b, pl.ds(0, CHIPS - 1)], 4, b)
        for c in range(2):
            lanes = slice(c * 128, (c + 1) * 128)
            flat[c] = back_in[b, :, :, lanes].reshape(512, 128).astype(F32)
            for s in range(4):
                pair_out[b, s // 2, s % 2, :, lanes] = flat[c, pl.ds(s, 128, stride=4), :].astype(
                    BF
                )
        remote(
            pair_out.at[b, 1 - core], back.at[b, :, half, :], 5, b, device(plane, partner)
        ).start()
        back[b, :, half, :] = pair_out[b, core]

    def finish(b):
        mean, scale = mixture_stats(4 + b)
        arrived(back.at[b, :, pl.ds(0, 128), :], 5, b)
        for s in range(2):
            normed = (back[b, s].astype(F32) - mean) * scale * ggain_ref[1:2] + gbias_ref[1:2]
            out_ref[b, s] = (normed + carried[b, s].astype(F32)).astype(BF)

    def step(t, _):
        def when(first, work, count=4):
            due = (t >= first) & (t <= first + 2 * count - 2) & (lax.rem(t, 2) == first % 2)
            pl.when(due)(lambda: work(lax.div(t - first, 2)))

        pl.when(t == 1)(lambda: loaded(1))
        pl.when(t == 2)(lambda: loaded(2))

        @pl.when(t == 8)
        def _():
            loaded(3)
            turn(1)

        unit = jnp.where(t < 8, t, t - (V_AT - 8))
        busy = (t < 8) | ((t >= V_AT) & (t < V_AT + 8))
        pl.when(busy & (lax.rem(t, 2) == 0))(lambda: first_half(unit))

        @pl.when(busy & (lax.rem(t, 2) == 1))
        def _():
            second_half(unit)
            pl.when(t == 1)(lambda: pl.semaphore_wait(barrier, COLUMN - 1 + PLANE - 1))
            start_stats(lax.div(unit, 2))
            pl.when(t >= V_AT)(lambda: send_back(lax.div(unit - 8, 2)))

        when(S2_AT, relay_stats)
        when(S2V_AT, lambda b: relay_stats(4 + b))
        when(N_AT, carry)
        when(R_AT, regroup)
        when(RR_AT, regroup_back)
        when(F_AT, finish)
        return 0

    loaded(0)
    turn(0)
    lax.fori_loop(0, F_AT + 7, step, 0)

    def drain(b, _):
        for slot in (b, 4 + b):
            left(stat_a.at[slot, pl.ds(0, COLUMN - 1)], 0, slot)
            left(stat_b.at[slot, pl.ds(0, PLANE - 1)], 1, slot)
        left(pair_in.at[b, 0], 2, b)
        left(chip_in.at[b, pl.ds(0, CHIPS - 1)], 3, b)
        left(back_in.at[b, pl.ds(0, CHIPS - 1)], 4, b)
        left(pair_out.at[b, 0], 5, b)
        return 0

    lax.fori_loop(0, MIX, drain, 0)


def on_device(mixture, w_attn, w_up, w_down, norm_gain, norm_bias, group_gain, group_bias):
    hbm = pl.BlockSpec(memory_space=pltpu.HBM)
    return pl.pallas_call(
        kernel,
        name="dual_path",
        out_shape=jax.ShapeDtypeStruct(mixture.shape, BF),
        in_specs=[hbm] * 9,
        out_specs=pl.BlockSpec(memory_space=pltpu.VMEM),
        scratch_shapes=[
            pltpu.VMEM((2, 4, D, D), BF),
            pltpu.VMEM((2, D, 4 * D), BF),
            pltpu.VMEM((2, 4 * D, D), BF),
            pltpu.VMEM((2, 2, D), F32),
            pltpu.VMEM((2, 2, D), F32),
            pltpu.VMEM((2, D), F32),
            pltpu.VMEM((2, D), F32),
            pltpu.VMEM((2, LENGTH, D), F32),
            pltpu.VMEM((MIX, 2, LENGTH, D), BF),
            pltpu.VMEM((2, 2 * D, D), BF),
            pltpu.VMEM((2, LENGTH, D), F32),
            pltpu.VMEM((MIX, 2, LENGTH, D), F32),
            pltpu.VMEM((MIX, 2, LENGTH, D), BF),
            pltpu.VMEM((MIX, 2, 2, 128, D), BF),
            pltpu.VMEM((MIX, CHIPS, 8, D), BF),
            pltpu.VMEM((MIX, CHIPS, 8, D), BF),
            pltpu.VMEM((MIX, CHIPS, 8, D), BF),
            pltpu.VMEM((MIX, CHIPS, 8, D), BF),
            pltpu.VMEM((MIX, 2, 2, 128, D), BF),
            pltpu.VMEM((MIX, 2, LENGTH, D), BF),
            pltpu.VMEM((2, 512, 128), F32),
            pltpu.VMEM((3, 8, D), F32),
            pltpu.VMEM((8, 8, 128), F32),
            pltpu.VMEM((8, COLUMN, 8, 128), F32),
            pltpu.VMEM((8, 8, 128), F32),
            pltpu.VMEM((8, PLANE, 8, 128), F32),
            pltpu.SemaphoreType.DMA((6, 8)),
            pltpu.SemaphoreType.DMA((6, 8)),
            pltpu.SemaphoreType.DMA((4, 5)),
        ],
        compiler_params=pltpu.CompilerParams(
            collective_id=0, has_side_effects=True, vmem_limit_bytes=60 * 1024 * 1024
        ),
    )(
        mixture, w_attn, w_up, w_down, norm_gain, norm_bias, group_gain, group_bias,
        jnp.asarray(position_tables()),
    )


def solution(mesh):
    split = P(None, ("wide", "narrow"), None, None)
    return jax.shard_map(
        on_device, mesh=mesh, in_specs=(split,) + (P(),) * 7, out_specs=split, check_vma=False
    )
```

```python
import math

import jax
import jax.numpy as jnp
import numpy as np
from jax import lax
from jax.experimental import pallas as pl
from jax.experimental.pallas import tpu as pltpu
from jax.sharding import PartitionSpec as P

F32 = jnp.float32
BF = jnp.bfloat16
MESH = pl.DeviceIdType.MESH

HEADS = 8
HEAD = 32
D = 256
LENGTH = 256
MIX = 4
PLANE = 16
COLUMN = 8
CHIPS = 64
EPSILON = 1e-05
QUERY_SCALE = math.log2(math.e) / math.sqrt(HEAD)
UNIT_CELLS = 2.0 * LENGTH * D
COLUMN_CELLS = UNIT_CELLS * COLUMN
MIX_CELLS = COLUMN_CELLS * PLANE
FAR_FIRST = sorted(
    range(1, CHIPS), key=lambda k: -sum((0, 1, 2, 1)[k // d % 4] for d in (1, 4, 16))
)
S2_AT = 4
V_AT = 14
N_AT = 7
R_AT = 8
RR_AT = 20
F_AT = 22
S2V_AT = 18
FIRST_AT = 2


def position_tables():
    positions = np.arange(LENGTH, dtype=np.float32)[:, None]
    freq = np.arange(D // 2, dtype=np.float32)[None, :]
    angles = positions * np.exp(freq * np.float32(-2.0 * math.log(10000.0) / D))
    table = np.concatenate([np.sin(angles), np.cos(angles)], axis=1).astype(np.float32)
    s, chip = np.meshgrid(np.arange(4), np.arange(CHIPS), indexing="ij")
    order = (4 * chip + s).reshape(-1)
    return np.stack([table, table[order]])


def dot(a, b):
    return jnp.dot(a, b, preferred_element_type=F32)


def layer_norm(rows, gain, bias):
    mean = jnp.mean(rows, axis=-1, keepdims=True)
    centered = rows - mean
    variance = jnp.mean(centered * centered, axis=-1, keepdims=True)
    return centered * lax.rsqrt(variance + EPSILON) * gain + bias


def attention(states, gain, bias, qv_t, wk, wo):
    normed = [layer_norm(state, gain, bias).astype(BF) for state in states]
    both = [
        lax.dot_general(qv_t, rows, (((1,), (1,)), ((), ())), preferred_element_type=F32)
        for rows in normed
    ]
    queries = [(part[:D] * QUERY_SCALE).astype(BF) for part in both]
    values = [part[D:].astype(BF) for part in both]
    keys = [dot(rows, wk).astype(BF) for rows in normed]
    ones = jnp.ones((16, LENGTH), BF)
    rows = [slice(h * HEAD, (h + 1) * HEAD) for h in range(HEADS)]
    scores = [dot(key[:, r], query[r]) for query, key in zip(queries, keys) for r in rows]
    weights = [jnp.exp2(part - jnp.max(part, axis=0, keepdims=True)).astype(BF) for part in scores]
    padded = [jnp.concatenate([value[r], ones], axis=0) for value in values for r in rows]
    summed = [dot(value, part) for value, part in zip(padded, weights)]
    heads = [(part[:HEAD] * (1.0 / part[HEAD : HEAD + 1])).astype(BF) for part in summed]
    after = [
        jnp.concatenate(heads[i : i + HEADS], axis=0).T for i in range(0, len(heads), HEADS)
    ]
    return [state + dot(rows, wo) for state, rows in zip(states, after)]


def feed_forward(afters, gain, bias, up, down):
    normed = [layer_norm(after, gain, bias).astype(BF) for after in afters]
    active = [jnp.maximum(dot(rows, up), 0.0).astype(BF) for rows in normed]
    return [after + dot(rows, down) for after, rows in zip(afters, active)]


def combine(total, spread, count, cells):
    whole = jnp.sum(total, axis=0, keepdims=True)
    offset = total - whole * (1.0 / count)
    square = jnp.sum(spread, axis=0, keepdims=True)
    return whole, square + jnp.sum(offset * offset, axis=0, keepdims=True) * (1.0 / cells)


def pack_stats(total, spread):
    row = lax.broadcasted_iota(jnp.int32, (8, 128), 0)
    wide_total = jnp.broadcast_to(total, (8, 128))
    return jnp.where(row == 0, wide_total, jnp.broadcast_to(spread, (8, 128)))


def kernel(
    mix_ref, attn_hbm, up_hbm, down_hbm, gain_hbm, bias_hbm, ggain_hbm, gbias_hbm, pos_hbm,
    out_ref,
    attn_ref, up_ref, down_ref, gain_ref, bias_ref, ggain_ref, gbias_ref, pos_ref,
    state, qv_t, middle, y, carried, pair_in, chip_out, chip_in, back_out, back_in, pair_out,
    back, flat, partial, stat_own, stat_a, stat_mid, stat_b, sent, recv, load_sem,
):
    index = lax.axis_index("wide") * 16 + lax.axis_index("narrow")
    plane = lax.div(index, 8)
    column = lax.rem(index, 8)
    chip = lax.div(index, 2)
    core = lax.rem(index, 2)
    partner = column + 1 - 2 * core
    half = pl.ds(pl.multiple_of(core * 128, 128), 128)
    other_half = pl.ds(pl.multiple_of(128 - core * 128, 128), 128)

    def device(p, r):
        return (lax.div(p, 2), lax.rem(p, 2) * 8 + r)

    def each_column(work):
        for k in range(1, COLUMN):
            work(lax.rem(column + k, COLUMN))

    def each_plane(work):
        for k in range(1, PLANE):
            work(lax.rem(plane + k, PLANE))

    def each_chip(work):
        for k in FAR_FIRST:
            x = lax.rem(lax.div(chip, 16) + k // 16, 4)
            y_ = lax.rem(lax.div(lax.rem(chip, 16), 4) + k // 4 % 4, 4)
            z = lax.rem(lax.rem(chip, 4) + k % 4, 4)
            work(x, y_, z)

    def chip_device(x, y_, z, c):
        return (x * 2 + lax.div(y_, 2), lax.rem(y_, 2) * 8 + z * 2 + c)

    def remote(src, dst, kind, slot, where):
        return pltpu.make_async_remote_copy(
            src_ref=src, dst_ref=dst, send_sem=sent.at[kind, slot], recv_sem=recv.at[kind, slot],
            device_id=where, device_id_type=MESH,
        )

    def arrived(ref, kind, slot):
        pltpu.make_async_copy(ref, ref, recv.at[kind, slot]).wait()

    def left(ref, kind, slot):
        pltpu.make_async_copy(ref, ref, sent.at[kind, slot]).wait()

    loads = (
        ((mix_ref.at[0], state.at[0]), (attn_hbm.at[0], attn_ref.at[0]),
         (gain_hbm, gain_ref), (bias_hbm, bias_ref), (pos_hbm.at[0], pos_ref.at[0])),
        ((up_hbm.at[0], up_ref.at[0]), (down_hbm.at[0], down_ref.at[0])),
        ((mix_ref.at[pl.ds(1, MIX - 1)], state.at[pl.ds(1, MIX - 1)]),
         (ggain_hbm, ggain_ref), (gbias_hbm, gbias_ref)),
        ((attn_hbm.at[1], attn_ref.at[1]), (pos_hbm.at[1], pos_ref.at[1]),
         (up_hbm.at[1], up_ref.at[1]), (down_hbm.at[1], down_ref.at[1])),
    )
    loads = [
        [pltpu.make_async_copy(src, dst, load_sem.at[i, j]) for j, (src, dst) in enumerate(group)]
        for i, group in enumerate(loads)
    ]
    for group in loads:
        for copy in group:
            copy.start()

    def loaded(i):
        for copy in loads[i]:
            copy.wait()

    barrier = pltpu.get_barrier_semaphore()

    def greet(where):
        pl.semaphore_signal(barrier, inc=1, device_id=where, device_id_type=MESH)

    each_column(lambda r: greet(device(plane, r)))
    each_plane(lambda p: greet(device(p, column)))

    def turn(l):
        for i, j in ((0, 0), (1, 2)):
            qv_t[l, i * D : (i + 1) * D] = attn_ref[l, j].T

    def first_half(t):
        l = lax.div(t, 8)
        b = lax.div(lax.rem(t, 8), 2)

        @pl.when(l == 0)
        def _():
            for s in range(2):
                middle[s] = state[b, s].astype(F32)

        @pl.when(l == 1)
        def _():
            arrived(chip_in.at[b, pl.ds(0, CHIPS - 1)], 3, b)
            for c in range(2):
                lanes = slice(c * 128, (c + 1) * 128)
                flat[c, :512] = chip_in[b, :, :, lanes].reshape(512, 128).astype(F32)
                for f in range(2):
                    for s in range(4):
                        middle[f, s * CHIPS : (s + 1) * CHIPS, lanes] = flat[
                            c, pl.ds(4 * f + s, CHIPS, stride=8), :
                        ]

        starts = [middle[s] + pos_ref[l] for s in range(2)]
        after = attention(
            starts, gain_ref[l, 0:1], bias_ref[l, 0:1], qv_t[l], attn_ref[l, 1], attn_ref[l, 3]
        )
        for s in range(2):
            middle[s] = after[s]

    def second_half(t):
        l = lax.div(t, 8)
        b = lax.div(lax.rem(t, 8), 2)
        afters = [middle[s] for s in range(2)]
        outs = feed_forward(
            afters, gain_ref[l, 1:2], bias_ref[l, 1:2], up_ref[l], down_ref[l]
        )
        pivot = None
        for s in range(2):
            out = jnp.where(l == 0, outs[s], outs[s].astype(BF).astype(F32))
            y[b, s] = out
            if pivot is None:
                pivot = out[:8]
                near = square = jnp.zeros((8, D), F32)
            offset = out.reshape(LENGTH // 8, 8, D) - pivot[None]
            near = near + jnp.sum(offset, axis=0)
            square = square + jnp.sum(offset * offset, axis=0)
        partial[lax.rem(b, 2), 0] = pivot
        partial[lax.rem(b, 2), 1] = near
        partial[lax.rem(b, 2), 2] = square

    def send_back(b):
        for c in range(2):
            lanes = slice(c * 128, (c + 1) * 128)
            for f in range(2):
                for s in range(4):
                    flat[c, pl.ds(4 * f + s, CHIPS, stride=8), :] = y[
                        b, f, s * CHIPS : (s + 1) * CHIPS, lanes
                    ]
            back_out[b, :, :, lanes] = flat[c, :512].reshape(CHIPS, 8, 128).astype(BF)
        back_in[b, chip] = back_out[b, chip]
        each_chip(
            lambda x, y_, z: remote(
                back_out.at[b, x * 16 + y_ * 4 + z], back_in.at[b, chip],
                4, b, chip_device(x, y_, z, core),
            ).start()
        )

    def start_stats(slot):
        start, near, square = (partial[lax.rem(slot, 2), i] for i in range(3))
        totals = near + start * 64.0
        spreads = square - near * near * (1.0 / 64.0)
        whole = jnp.sum(jnp.sum(totals, axis=0, keepdims=True), axis=1, keepdims=True)
        offset = totals - whole * (1.0 / 2048.0)
        spreads = spreads + offset * offset * (1.0 / 64.0)
        spread = jnp.sum(jnp.sum(spreads, axis=0, keepdims=True), axis=1, keepdims=True)
        packed = pack_stats(whole, spread)
        stat_own[slot] = packed
        stat_a[slot, column] = packed
        each_column(
            lambda r: remote(
                stat_own.at[slot], stat_a.at[slot, column], 0, slot, device(plane, r)
            ).start()
        )

    def relay_stats(slot):
        arrived(stat_a.at[slot, pl.ds(0, COLUMN - 1)], 0, slot)
        total, spread = combine(stat_a[slot, :, 0, :], stat_a[slot, :, 1, :], COLUMN, UNIT_CELLS)
        packed = pack_stats(total, spread)
        stat_mid[slot] = packed
        stat_b[slot, plane] = packed
        each_plane(
            lambda p: remote(
                stat_mid.at[slot], stat_b.at[slot, plane], 1, slot, device(p, column)
            ).start()
        )

    def mixture_stats(slot):
        arrived(stat_b.at[slot, pl.ds(0, PLANE - 1)], 1, slot)
        total, spread = combine(stat_b[slot, :, 0, :], stat_b[slot, :, 1, :], PLANE, COLUMN_CELLS)
        mean = total * (1.0 / MIX_CELLS)
        scale = lax.rsqrt(spread * (1.0 / MIX_CELLS) + EPSILON)
        return (
            jnp.concatenate([mean, mean], axis=1),
            jnp.concatenate([scale, scale], axis=1),
        )

    def carry(b):
        mean, scale = mixture_stats(b)
        for s in range(2):
            normed = (y[b, s] - mean) * scale * ggain_ref[0:1] + gbias_ref[0:1]
            carried[b, s] = (normed + state[b, s].astype(F32)).astype(BF)
        remote(
            carried.at[b, :, other_half, :], pair_in.at[b, core], 2, b, device(plane, partner)
        ).start()
        pair_in[b, core] = carried[b, :, half, :]

    def regroup(b):
        arrived(pair_in.at[b, 0], 2, b)
        for c in range(2):
            lanes = slice(c * 128, (c + 1) * 128)
            for s in range(4):
                flat[c, pl.ds(s, 128, stride=4), :] = pair_in[b, s // 2, s % 2, :, lanes].astype(
                    F32
                )
            chip_out[b, :, :, lanes] = flat[c, :512].reshape(CHIPS, 8, 128).astype(BF)
        chip_in[b, chip] = chip_out[b, chip]
        each_chip(
            lambda x, y_, z: remote(
                chip_out.at[b, x * 16 + y_ * 4 + z], chip_in.at[b, chip],
                3, b, chip_device(x, y_, z, core),
            ).start()
        )

    def regroup_back(b):
        arrived(back_in.at[b, pl.ds(0, CHIPS - 1)], 4, b)
        for c in range(2):
            lanes = slice(c * 128, (c + 1) * 128)
            flat[c, :512] = back_in[b, :, :, lanes].reshape(512, 128).astype(F32)
            for s in range(4):
                pair_out[b, s // 2, s % 2, :, lanes] = flat[c, pl.ds(s, 128, stride=4), :].astype(
                    BF
                )
        remote(
            pair_out.at[b, 1 - core], back.at[b, :, half, :], 5, b, device(plane, partner)
        ).start()
        back[b, :, half, :] = pair_out[b, core]

    def finish(b):
        mean, scale = mixture_stats(4 + b)
        arrived(back.at[b, :, pl.ds(0, 128), :], 5, b)
        for s in range(2):
            normed = (back[b, s].astype(F32) - mean) * scale * ggain_ref[1:2] + gbias_ref[1:2]
            out_ref[b, s] = (normed + carried[b, s].astype(F32)).astype(BF)

    def step(t, _):
        def when(first, work, count=4):
            due = (t >= first) & (t <= first + 2 * count - 2) & (lax.rem(t, 2) == first % 2)
            pl.when(due)(lambda: work(lax.div(t - first, 2)))

        pl.when(t == 1)(lambda: loaded(1))
        pl.when(t == 2)(lambda: loaded(2))

        @pl.when(t == 8)
        def _():
            loaded(3)
            turn(1)

        unit = jnp.where(t < 8, t, t - (V_AT - 8))
        busy = (t < 8) | ((t >= V_AT) & (t < V_AT + 8))
        pl.when(busy & (lax.rem(t, 2) == 0))(lambda: first_half(unit))

        @pl.when(t == FIRST_AT)
        def _():
            pl.semaphore_wait(barrier, COLUMN - 1 + PLANE - 1)
            start_stats(0)

        @pl.when(busy & (lax.rem(t, 2) == 1))
        def _():
            second_half(unit)
            pl.when(t != 1)(lambda: start_stats(lax.div(unit, 2)))
            pl.when(t >= V_AT)(lambda: send_back(lax.div(unit - 8, 2)))

        when(S2_AT, relay_stats)
        when(S2V_AT, lambda b: relay_stats(4 + b))
        when(N_AT, carry)
        when(R_AT, regroup)
        when(RR_AT, regroup_back)
        when(F_AT, finish)
        return 0

    loaded(0)
    turn(0)
    lax.fori_loop(0, F_AT + 7, step, 0)

    def drain(b, _):
        for slot in (b, 4 + b):
            left(stat_a.at[slot, pl.ds(0, COLUMN - 1)], 0, slot)
            left(stat_b.at[slot, pl.ds(0, PLANE - 1)], 1, slot)
        left(pair_in.at[b, 0], 2, b)
        left(chip_in.at[b, pl.ds(0, CHIPS - 1)], 3, b)
        left(back_in.at[b, pl.ds(0, CHIPS - 1)], 4, b)
        left(pair_out.at[b, 0], 5, b)
        return 0

    lax.fori_loop(0, MIX, drain, 0)


def on_device(mixture, w_attn, w_up, w_down, norm_gain, norm_bias, group_gain, group_bias):
    hbm = pl.BlockSpec(memory_space=pltpu.HBM)
    return pl.pallas_call(
        kernel,
        name="dual_path",
        out_shape=jax.ShapeDtypeStruct(mixture.shape, BF),
        in_specs=[hbm] * 9,
        out_specs=pl.BlockSpec(memory_space=pltpu.VMEM),
        scratch_shapes=[
            pltpu.VMEM((2, 4, D, D), BF),
            pltpu.VMEM((2, D, 4 * D), BF),
            pltpu.VMEM((2, 4 * D, D), BF),
            pltpu.VMEM((2, 2, D), F32),
            pltpu.VMEM((2, 2, D), F32),
            pltpu.VMEM((2, D), F32),
            pltpu.VMEM((2, D), F32),
            pltpu.VMEM((2, LENGTH, D), F32),
            pltpu.VMEM((MIX, 2, LENGTH, D), BF),
            pltpu.VMEM((2, 2 * D, D), BF),
            pltpu.VMEM((2, LENGTH, D), F32),
            pltpu.VMEM((MIX, 2, LENGTH, D), F32),
            pltpu.VMEM((MIX, 2, LENGTH, D), BF),
            pltpu.VMEM((MIX, 2, 2, 128, D), BF),
            pltpu.VMEM((MIX, CHIPS, 8, D), BF),
            pltpu.VMEM((MIX, CHIPS, 8, D), BF),
            pltpu.VMEM((MIX, CHIPS, 8, D), BF),
            pltpu.VMEM((MIX, CHIPS, 8, D), BF),
            pltpu.VMEM((MIX, 2, 2, 128, D), BF),
            pltpu.VMEM((MIX, 2, LENGTH, D), BF),
            pltpu.VMEM((2, 520, 128), F32),
            pltpu.VMEM((2, 3, 8, D), F32),
            pltpu.VMEM((8, 8, 128), F32),
            pltpu.VMEM((8, COLUMN, 8, 128), F32),
            pltpu.VMEM((8, 8, 128), F32),
            pltpu.VMEM((8, PLANE, 8, 128), F32),
            pltpu.SemaphoreType.DMA((6, 8)),
            pltpu.SemaphoreType.DMA((6, 8)),
            pltpu.SemaphoreType.DMA((4, 5)),
        ],
        compiler_params=pltpu.CompilerParams(
            collective_id=0, has_side_effects=True, vmem_limit_bytes=60 * 1024 * 1024
        ),
    )(
        mixture, w_attn, w_up, w_down, norm_gain, norm_bias, group_gain, group_bias,
        jnp.asarray(position_tables()),
    )


def solution(mesh):
    split = P(None, ("wide", "narrow"), None, None)
    return jax.shard_map(
        on_device, mesh=mesh, in_specs=(split,) + (P(),) * 7, out_specs=split, check_vma=False
    )
```

```python
import math

import jax
import jax.numpy as jnp
import numpy as np
from jax import lax
from jax.experimental import pallas as pl
from jax.experimental.pallas import tpu as pltpu
from jax.sharding import PartitionSpec as P

F32 = jnp.float32
BF = jnp.bfloat16
MESH = pl.DeviceIdType.MESH

HEADS = 8
HEAD = 32
D = 256
LENGTH = 256
MIX = 4
PLANE = 16
COLUMN = 8
CHIPS = 64
EPSILON = 1e-05
QUERY_SCALE = math.log2(math.e) / math.sqrt(HEAD)
UNIT_CELLS = 2.0 * LENGTH * D
COLUMN_CELLS = UNIT_CELLS * COLUMN
MIX_CELLS = COLUMN_CELLS * PLANE
FAR_FIRST = sorted(
    range(1, CHIPS), key=lambda k: -sum((0, 1, 2, 1)[k // d % 4] for d in (1, 4, 16))
)
S2_AT = 4
V_AT = 14
N_AT = 7
R_AT = 8
RR_AT = 20
F_AT = 22
S2V_AT = 18
FIRST_AT = 2


def position_tables():
    positions = np.arange(LENGTH, dtype=np.float32)[:, None]
    freq = np.arange(D // 2, dtype=np.float32)[None, :]
    angles = positions * np.exp(freq * np.float32(-2.0 * math.log(10000.0) / D))
    table = np.concatenate([np.sin(angles), np.cos(angles)], axis=1).astype(np.float32)
    s, chip = np.meshgrid(np.arange(4), np.arange(CHIPS), indexing="ij")
    order = (4 * chip + s).reshape(-1)
    return np.stack([table, table[order]])


def dot(a, b):
    return jnp.dot(a, b, preferred_element_type=F32)


def layer_norm(rows, gain, bias):
    mean = jnp.mean(rows, axis=-1, keepdims=True)
    centered = rows - mean
    variance = jnp.mean(centered * centered, axis=-1, keepdims=True)
    return centered * lax.rsqrt(variance + EPSILON) * gain + bias


def attention(states, gain, bias, qv_t, wk, wo):
    normed = [layer_norm(state, gain, bias).astype(BF) for state in states]
    both = [
        lax.dot_general(qv_t, rows, (((1,), (1,)), ((), ())), preferred_element_type=F32)
        for rows in normed
    ]
    queries = [(part[:D] * QUERY_SCALE).astype(BF) for part in both]
    values = [part[D:].astype(BF) for part in both]
    keys = [dot(rows, wk).astype(BF) for rows in normed]
    ones = jnp.ones((16, LENGTH), BF)
    rows = [slice(h * HEAD, (h + 1) * HEAD) for h in range(HEADS)]
    scores = [dot(key[:, r], query[r]) for query, key in zip(queries, keys) for r in rows]
    weights = [jnp.exp2(part - jnp.max(part, axis=0, keepdims=True)).astype(BF) for part in scores]
    padded = [jnp.concatenate([value[r], ones], axis=0) for value in values for r in rows]
    summed = [dot(value, part) for value, part in zip(padded, weights)]
    heads = [(part[:HEAD] * (1.0 / part[HEAD : HEAD + 1])).astype(BF) for part in summed]
    after = [
        jnp.concatenate(heads[i : i + HEADS], axis=0).T for i in range(0, len(heads), HEADS)
    ]
    return [state + dot(rows, wo) for state, rows in zip(states, after)]


def feed_forward(afters, gain, bias, up, down):
    normed = [layer_norm(after, gain, bias).astype(BF) for after in afters]
    active = [jnp.maximum(dot(rows, up), 0.0).astype(BF) for rows in normed]
    return [after + dot(rows, down) for after, rows in zip(afters, active)]


def combine(total, spread, count, cells):
    whole = jnp.sum(total, axis=0, keepdims=True)
    offset = total - whole * (1.0 / count)
    square = jnp.sum(spread, axis=0, keepdims=True)
    return whole, square + jnp.sum(offset * offset, axis=0, keepdims=True) * (1.0 / cells)


def pack_stats(total, spread):
    row = lax.broadcasted_iota(jnp.int32, (8, 128), 0)
    wide_total = jnp.broadcast_to(total, (8, 128))
    return jnp.where(row == 0, wide_total, jnp.broadcast_to(spread, (8, 128)))


def kernel(
    mix_ref, attn_hbm, up_hbm, down_hbm, gain_hbm, bias_hbm, ggain_hbm, gbias_hbm, pos_hbm,
    out_ref,
    attn_ref, up_ref, down_ref, gain_ref, bias_ref, ggain_ref, gbias_ref, pos_ref,
    state, qv_t, middle, y, carried, pair_in, chip_out, chip_in, back_out, back_in, pair_out,
    back, flat, partial, stat_own, stat_a, stat_mid, stat_b, sent, recv, load_sem,
):
    index = lax.axis_index("wide") * 16 + lax.axis_index("narrow")
    plane = lax.div(index, 8)
    column = lax.rem(index, 8)
    chip = lax.div(index, 2)
    core = lax.rem(index, 2)
    partner = column + 1 - 2 * core
    half = pl.ds(pl.multiple_of(core * 128, 128), 128)
    other_half = pl.ds(pl.multiple_of(128 - core * 128, 128), 128)

    def device(p, r):
        return (lax.div(p, 2), lax.rem(p, 2) * 8 + r)

    def each_column(work):
        for k in range(1, COLUMN):
            work(lax.rem(column + k, COLUMN))

    def each_plane(work):
        for k in range(1, PLANE):
            work(lax.rem(plane + k, PLANE))

    def each_chip(work):
        for k in FAR_FIRST:
            x = lax.rem(lax.div(chip, 16) + k // 16, 4)
            y_ = lax.rem(lax.div(lax.rem(chip, 16), 4) + k // 4 % 4, 4)
            z = lax.rem(lax.rem(chip, 4) + k % 4, 4)
            work(x, y_, z)

    def chip_device(x, y_, z, c):
        return (x * 2 + lax.div(y_, 2), lax.rem(y_, 2) * 8 + z * 2 + c)

    def remote(src, dst, kind, slot, where):
        return pltpu.make_async_remote_copy(
            src_ref=src, dst_ref=dst, send_sem=sent.at[kind, slot], recv_sem=recv.at[kind, slot],
            device_id=where, device_id_type=MESH,
        )

    def arrived(ref, kind, slot):
        pltpu.make_async_copy(ref, ref, recv.at[kind, slot]).wait()

    def left(ref, kind, slot):
        pltpu.make_async_copy(ref, ref, sent.at[kind, slot]).wait()

    loads = (
        ((mix_ref.at[0], state.at[0]), (attn_hbm.at[0], attn_ref.at[0]),
         (gain_hbm, gain_ref), (bias_hbm, bias_ref), (pos_hbm.at[0], pos_ref.at[0])),
        ((up_hbm.at[0], up_ref.at[0]), (down_hbm.at[0], down_ref.at[0])),
        ((mix_ref.at[pl.ds(1, MIX - 1)], state.at[pl.ds(1, MIX - 1)]),
         (ggain_hbm, ggain_ref), (gbias_hbm, gbias_ref)),
        ((attn_hbm.at[1], attn_ref.at[1]), (pos_hbm.at[1], pos_ref.at[1]),
         (up_hbm.at[1], up_ref.at[1]), (down_hbm.at[1], down_ref.at[1])),
    )
    loads = [
        [pltpu.make_async_copy(src, dst, load_sem.at[i, j]) for j, (src, dst) in enumerate(group)]
        for i, group in enumerate(loads)
    ]
    for group in loads:
        for copy in group:
            copy.start()

    def loaded(i):
        for copy in loads[i]:
            copy.wait()

    barrier = pltpu.get_barrier_semaphore()

    def greet(where):
        pl.semaphore_signal(barrier, inc=1, device_id=where, device_id_type=MESH)

    each_column(lambda r: greet(device(plane, r)))
    each_plane(lambda p: greet(device(p, column)))

    def turn(l):
        for i, j in ((0, 0), (1, 2)):
            qv_t[l, i * D : (i + 1) * D] = attn_ref[l, j].T

    def first_half(t):
        l = lax.div(t, 8)
        b = lax.div(lax.rem(t, 8), 2)

        @pl.when(l == 0)
        def _():
            for s in range(2):
                middle[s] = state[b, s].astype(F32)

        @pl.when(l == 1)
        def _():
            arrived(chip_in.at[b, pl.ds(0, CHIPS - 1)], 3, b)
            for c in range(2):
                lanes = slice(c * 128, (c + 1) * 128)
                flat[c, :512] = chip_in[b, :, :, lanes].reshape(512, 128).astype(F32)
                for f in range(2):
                    for s in range(4):
                        middle[f, s * CHIPS : (s + 1) * CHIPS, lanes] = flat[
                            c, pl.ds(4 * f + s, CHIPS, stride=8), :
                        ]

        starts = [middle[s] + pos_ref[l] for s in range(2)]
        after = attention(
            starts, gain_ref[l, 0:1], bias_ref[l, 0:1], qv_t[l], attn_ref[l, 1], attn_ref[l, 3]
        )
        for s in range(2):
            middle[s] = after[s]

    def second_half(t):
        l = lax.div(t, 8)
        b = lax.div(lax.rem(t, 8), 2)
        afters = [middle[s] for s in range(2)]
        outs = feed_forward(
            afters, gain_ref[l, 1:2], bias_ref[l, 1:2], up_ref[l], down_ref[l]
        )
        pivot = None
        for s in range(2):
            out = jnp.where(l == 0, outs[s], outs[s].astype(BF).astype(F32))
            y[b, s] = out
            if pivot is None:
                pivot = out[:8]
                near = square = jnp.zeros((8, D), F32)
            offset = out.reshape(LENGTH // 8, 8, D) - pivot[None]
            near = near + jnp.sum(offset, axis=0)
            square = square + jnp.sum(offset * offset, axis=0)
        partial[lax.rem(b, 2), 0] = pivot
        partial[lax.rem(b, 2), 1] = near
        partial[lax.rem(b, 2), 2] = square

    def send_back(b):
        for c in range(2):
            lanes = slice(c * 128, (c + 1) * 128)
            for f in range(2):
                for s in range(4):
                    flat[c, pl.ds(4 * f + s, CHIPS, stride=8), :] = y[
                        b, f, s * CHIPS : (s + 1) * CHIPS, lanes
                    ]
            back_out[b, :, :, lanes] = flat[c, :512].reshape(CHIPS, 8, 128).astype(BF)
        back_in[b, chip] = back_out[b, chip]
        each_chip(
            lambda x, y_, z: remote(
                back_out.at[b, x * 16 + y_ * 4 + z], back_in.at[b, chip],
                4, b, chip_device(x, y_, z, core),
            ).start()
        )

    def start_stats(slot):
        start, near, square = (partial[lax.rem(slot, 2), i] for i in range(3))
        totals = near + start * 64.0
        spreads = square - near * near * (1.0 / 64.0)
        whole = jnp.sum(jnp.sum(totals, axis=0, keepdims=True), axis=1, keepdims=True)
        offset = totals - whole * (1.0 / 2048.0)
        spreads = spreads + offset * offset * (1.0 / 64.0)
        spread = jnp.sum(jnp.sum(spreads, axis=0, keepdims=True), axis=1, keepdims=True)
        packed = pack_stats(whole, spread)
        stat_own[slot] = packed
        stat_a[slot, column] = packed
        each_column(
            lambda r: remote(
                stat_own.at[slot], stat_a.at[slot, column], 0, slot, device(plane, r)
            ).start()
        )

    def relay_stats(slot):
        arrived(stat_a.at[slot, pl.ds(0, COLUMN - 1)], 0, slot)
        total, spread = combine(stat_a[slot, :, 0, :], stat_a[slot, :, 1, :], COLUMN, UNIT_CELLS)
        packed = pack_stats(total, spread)
        stat_mid[slot] = packed
        stat_b[slot, plane] = packed
        each_plane(
            lambda p: remote(
                stat_mid.at[slot], stat_b.at[slot, plane], 1, slot, device(p, column)
            ).start()
        )

    def mixture_stats(slot):
        arrived(stat_b.at[slot, pl.ds(0, PLANE - 1)], 1, slot)
        total, spread = combine(stat_b[slot, :, 0, :], stat_b[slot, :, 1, :], PLANE, COLUMN_CELLS)
        mean = total * (1.0 / MIX_CELLS)
        scale = lax.rsqrt(spread * (1.0 / MIX_CELLS) + EPSILON)
        return (
            jnp.concatenate([mean, mean], axis=1),
            jnp.concatenate([scale, scale], axis=1),
        )

    def carry(b):
        mean, scale = mixture_stats(b)
        for s in range(2):
            normed = (y[b, s] - mean) * scale * ggain_ref[0:1] + gbias_ref[0:1]
            carried[b, s] = (normed + state[b, s].astype(F32)).astype(BF)
        remote(
            carried.at[b, :, other_half, :], pair_in.at[b, core], 2, b, device(plane, partner)
        ).start()
        pair_in[b, core] = carried[b, :, half, :]

    def regroup(b):
        arrived(pair_in.at[b, 0], 2, b)
        for c in range(2):
            lanes = slice(c * 128, (c + 1) * 128)
            for s in range(4):
                flat[c, pl.ds(s, 128, stride=4), :] = pair_in[b, s // 2, s % 2, :, lanes].astype(
                    F32
                )
            chip_out[b, :, :, lanes] = flat[c, :512].reshape(CHIPS, 8, 128).astype(BF)
        chip_in[b, chip] = chip_out[b, chip]
        each_chip(
            lambda x, y_, z: remote(
                chip_out.at[b, x * 16 + y_ * 4 + z], chip_in.at[b, chip],
                3, b, chip_device(x, y_, z, core),
            ).start()
        )

    def regroup_back(b):
        arrived(back_in.at[b, pl.ds(0, CHIPS - 1)], 4, b)
        for c in range(2):
            lanes = slice(c * 128, (c + 1) * 128)
            flat[c, :512] = back_in[b, :, :, lanes].reshape(512, 128).astype(F32)
            for s in range(4):
                pair_out[b, s // 2, s % 2, :, lanes] = flat[c, pl.ds(s, 128, stride=4), :].astype(
                    BF
                )
        remote(
            pair_out.at[b, 1 - core], back.at[b, :, half, :], 5, b, device(plane, partner)
        ).start()
        back[b, :, half, :] = pair_out[b, core]

    def finish(b):
        mean, scale = mixture_stats(4 + b)
        arrived(back.at[b, :, pl.ds(0, 128), :], 5, b)
        for s in range(2):
            normed = (back[b, s].astype(F32) - mean) * scale * ggain_ref[1:2] + gbias_ref[1:2]
            out_ref[b, s] = (normed + carried[b, s].astype(F32)).astype(BF)

    def step(t, _):
        def when(first, work, count=4):
            due = (t >= first) & (t <= first + 2 * count - 2) & (lax.rem(t, 2) == first % 2)
            pl.when(due)(lambda: work(lax.div(t - first, 2)))

        pl.when(t == 1)(lambda: loaded(1))
        pl.when(t == 2)(lambda: loaded(2))

        @pl.when(t == 8)
        def _():
            loaded(3)
            turn(1)

        unit = jnp.where(t < 8, t, t - (V_AT - 8))
        busy = (t < 8) | ((t >= V_AT) & (t < V_AT + 8))
        pl.when(busy & (lax.rem(t, 2) == 0))(lambda: first_half(unit))

        @pl.when(t == FIRST_AT)
        def _():
            pl.semaphore_wait(barrier, COLUMN - 1 + PLANE - 1)
            start_stats(0)

        @pl.when(busy & (lax.rem(t, 2) == 1))
        def _():
            second_half(unit)
            pl.when(t != 1)(lambda: start_stats(lax.div(unit, 2)))
            pl.when(t >= V_AT)(lambda: send_back(lax.div(unit - 8, 2)))

        when(S2_AT, relay_stats)
        when(S2V_AT, lambda b: relay_stats(4 + b), 3)
        pl.when(t == 23)(lambda: relay_stats(7))
        when(N_AT, carry)
        when(R_AT, regroup)
        when(RR_AT, regroup_back)
        when(F_AT, finish)
        return 0

    loaded(0)
    turn(0)
    lax.fori_loop(0, F_AT + 7, step, 0)

    def drain(b, _):
        for slot in (b, 4 + b):
            left(stat_a.at[slot, pl.ds(0, COLUMN - 1)], 0, slot)
            left(stat_b.at[slot, pl.ds(0, PLANE - 1)], 1, slot)
        left(pair_in.at[b, 0], 2, b)
        left(chip_in.at[b, pl.ds(0, CHIPS - 1)], 3, b)
        left(back_in.at[b, pl.ds(0, CHIPS - 1)], 4, b)
        left(pair_out.at[b, 0], 5, b)
        return 0

    lax.fori_loop(0, MIX, drain, 0)


def on_device(mixture, w_attn, w_up, w_down, norm_gain, norm_bias, group_gain, group_bias):
    hbm = pl.BlockSpec(memory_space=pltpu.HBM)
    return pl.pallas_call(
        kernel,
        name="dual_path",
        out_shape=jax.ShapeDtypeStruct(mixture.shape, BF),
        in_specs=[hbm] * 9,
        out_specs=pl.BlockSpec(memory_space=pltpu.VMEM),
        scratch_shapes=[
            pltpu.VMEM((2, 4, D, D), BF),
            pltpu.VMEM((2, D, 4 * D), BF),
            pltpu.VMEM((2, 4 * D, D), BF),
            pltpu.VMEM((2, 2, D), F32),
            pltpu.VMEM((2, 2, D), F32),
            pltpu.VMEM((2, D), F32),
            pltpu.VMEM((2, D), F32),
            pltpu.VMEM((2, LENGTH, D), F32),
            pltpu.VMEM((MIX, 2, LENGTH, D), BF),
            pltpu.VMEM((2, 2 * D, D), BF),
            pltpu.VMEM((2, LENGTH, D), F32),
            pltpu.VMEM((MIX, 2, LENGTH, D), F32),
            pltpu.VMEM((MIX, 2, LENGTH, D), BF),
            pltpu.VMEM((MIX, 2, 2, 128, D), BF),
            pltpu.VMEM((MIX, CHIPS, 8, D), BF),
            pltpu.VMEM((MIX, CHIPS, 8, D), BF),
            pltpu.VMEM((MIX, CHIPS, 8, D), BF),
            pltpu.VMEM((MIX, CHIPS, 8, D), BF),
            pltpu.VMEM((MIX, 2, 2, 128, D), BF),
            pltpu.VMEM((MIX, 2, LENGTH, D), BF),
            pltpu.VMEM((2, 520, 128), F32),
            pltpu.VMEM((2, 3, 8, D), F32),
            pltpu.VMEM((8, 8, 128), F32),
            pltpu.VMEM((8, COLUMN, 8, 128), F32),
            pltpu.VMEM((8, 8, 128), F32),
            pltpu.VMEM((8, PLANE, 8, 128), F32),
            pltpu.SemaphoreType.DMA((6, 8)),
            pltpu.SemaphoreType.DMA((6, 8)),
            pltpu.SemaphoreType.DMA((4, 5)),
        ],
        compiler_params=pltpu.CompilerParams(
            collective_id=0, has_side_effects=True, vmem_limit_bytes=60 * 1024 * 1024
        ),
    )(
        mixture, w_attn, w_up, w_down, norm_gain, norm_bias, group_gain, group_bias,
        jnp.asarray(position_tables()),
    )


def solution(mesh):
    split = P(None, ("wide", "narrow"), None, None)
    return jax.shard_map(
        on_device, mesh=mesh, in_specs=(split,) + (P(),) * 7, out_specs=split, check_vma=False
    )
```
